128 devices in a mesh: gx: 8 (over y_lo, x), gy: 8 (over z, core), gz: 2 (over y_hi).
Axes of the slice: x: 4, y: 4 (y_hi: 2, y_lo: 2; y = y_hi * 2 + y_lo), z: 4, core: 2. Of those that a mesh axis runs over, the one named last changes fastest.
Arguments:
- blocks: int32 [131072, 4], P(('gx', 'gy', 'gz')), may hold values from 0 to 15, as said below
- coefficients: bfloat16 [131072, 4, 128], P(('gx', 'gy', 'gz')), may hold values from -80 to 80
- residuals: float32 [131072], P(('gx', 'gy', 'gz')), may hold values from -3000 to 3000
Outputs:
- factor: float32 [8, 2, 128, 8, 2, 128], P('gx', None, None, 'gy')
- solution: float32 [16, 128], replicated
The draws below stay inside these ranges and needn't reach their ends.
Inputs may be any that keep to these rules, and one draw needn't show every extreme that they name: Each row names 4 different blocks.
All inputs are finite; a program needn't handle non-finite values.
Results may differ from the reference program's by a relative error of at most 0.0003.
Values sent between devices are 32-bit elements; how exact they have to be, the bound alone decides.
A program may use at most 128 MiB of HBM per device.

```python
import math
import jax
import jax.numpy as jnp
from jax import lax

G = 2048
BS = 128
SLOTS = 4
OBS = 131072
N_GX = 8
N_GY = 8


def pick_blocks(key):
    nblock = G // BS
    base = jax.random.fold_in(key, 11)
    scores = jax.random.randint(base, (OBS, nblock), 0, 1 << 20) * nblock + jnp.arange(nblock, dtype=jnp.int32)[None, :]
    chosen = lax.top_k(scores, SLOTS)[1]
    return chosen.astype(jnp.int32)


def make_coefficients(key):
    base = jax.random.fold_in(key, 23)
    noise = jnp.clip(jax.random.normal(jax.random.fold_in(base, 1), (OBS, SLOTS, BS), jnp.float32), -6.0, 6.0)
    mixing = jax.random.normal(jax.random.fold_in(base, 3), (BS, BS), jnp.float32) / math.sqrt(BS)
    neighbour = jnp.roll(noise, -1, axis=1)
    coupled = noise + 0.35 * jnp.einsum('osx,xy->osy', neighbour, mixing)
    return jnp.clip(coupled, -80.0, 80.0)


def draw_blocks(key, part):
    return pick_blocks(key)


def draw_coefficients(key, part):
    return make_coefficients(key).astype(jnp.bfloat16)


def draw_residuals(key, part):
    coef = make_coefficients(key)
    chosen = pick_blocks(key)
    truth = jax.random.normal(jax.random.fold_in(key, 37), (G // BS, BS), jnp.float32)
    picked = truth[chosen]
    noise = jax.random.normal(jax.random.fold_in(key, 41), (OBS,), jnp.float32)
    values = jnp.sum(coef * picked, axis=(1, 2)) + noise
    return jnp.clip(values, -3000.0, 3000.0)


def setup_inputs(seed: int = 0) -> dict:
    key_list = jax.random.split(jax.random.key(seed), 4)
    blocks = draw_blocks(jax.random.fold_in(key_list[3], 71), 0)
    coefficients = draw_coefficients(jax.random.fold_in(key_list[3], 71), 0)
    residuals = draw_residuals(jax.random.fold_in(key_list[3], 71), 0)
    return {"blocks": blocks, "coefficients": coefficients, "residuals": residuals}


def reference(blocks, coefficients, residuals):
    total = blocks.shape[0]
    nblock = G // BS
    per_dev = nblock // N_GX
    group = math.gcd(total, 4096)
    count = total // group
    labels = jnp.arange(nblock, dtype=jnp.int32)

    def accumulate(carry, index):
        start = (index * group).astype(jnp.int32)
        picked = lax.dynamic_slice_in_dim(blocks, start, group, 0)
        coef = lax.dynamic_slice_in_dim(coefficients, start, group, 0).astype(jnp.float32)
        resid = lax.dynamic_slice_in_dim(residuals, start, group, 0)
        placed = (picked[:, :, None] == labels[None, None, :]).astype(jnp.float32)
        design = jnp.einsum('osa,osx->oax', placed, coef, precision=lax.Precision.HIGHEST).reshape(group, G)
        normal = carry[0] + jnp.dot(design.T.astype(jnp.float32), design.astype(jnp.float32), precision=lax.Precision.HIGHEST, preferred_element_type=jnp.float32)
        rhs = carry[1] + jnp.dot(resid.astype(jnp.float32), design.astype(jnp.float32), precision=lax.Precision.HIGHEST, preferred_element_type=jnp.float32)
        return ((normal, rhs), None)
    start_state = (jnp.zeros((G, G), jnp.float32), jnp.zeros((G,), jnp.float32))
    (normal, rhs), _ = lax.scan(accumulate, start_state, jnp.arange(count, dtype=jnp.int32))
    normal = normal / total
    rhs = rhs / total
    lower = jnp.linalg.cholesky(normal)
    middle = jax.scipy.linalg.solve_triangular(lower, rhs, lower=True)
    answer = jax.scipy.linalg.solve_triangular(lower.T, middle, lower=False)
    factor = lower.reshape(per_dev, N_GX, BS, per_dev, N_GY, BS).transpose(1, 0, 2, 4, 3, 5)
    return (factor, answer.reshape(nblock, BS))
```

```python
import functools

import jax
import jax.numpy as jnp
from jax import lax
from jax.experimental import pallas as pl
from jax.experimental.pallas import tpu as pltpu
from jax.sharding import PartitionSpec as P

G = 2048
BS = 128
SB = 2 * BS
SUB = 8
VMEM_LIMIT = 60 * 1024 * 1024


def mm(a, b, ca, cb, precision=lax.Precision.HIGHEST):
    return lax.dot_general(
        a, b, (((ca,), (cb,)), ((), ())), precision=precision, preferred_element_type=jnp.float32
    )


def split(x):
    high = x.astype(jnp.bfloat16)
    return high, (x - high.astype(jnp.float32)).astype(jnp.bfloat16)


def mm3(a, b, ca, cb):
    (ah, al), (bh, bl) = split(a), b if isinstance(b, tuple) else split(b)
    return mm(ah, bh, ca, cb, None) + (mm(ah, bl, ca, cb, None) + mm(al, bh, ca, cb, None))


def panel_start(nblock, k):
    return BS * (nblock * k - (k * (k - 1)) // 2)


def gram_kernel(nblock, scale, blocks_ref, coef_ref, res_ref, out_ref, design):
    slots = coef_ref.shape[0]
    rows = coef_ref.shape[1]
    chunk = 128
    nsuper = nblock // 2

    @pl.loop(0, rows // chunk)
    def _(t):
        at = pl.ds(pl.multiple_of(t * chunk, chunk), chunk)
        idx = blocks_ref[at, :]
        labels = [jnp.broadcast_to(idx[:, s : s + 1], (chunk, BS)) for s in range(slots)]
        values = [coef_ref[s, at, :].astype(jnp.float32) for s in range(slots)]
        for b in range(nblock):
            total = jnp.where(labels[0] == b, values[0], 0.0)
            for s in range(1, slots):
                total = jnp.where(labels[s] == b, values[s], total)
            design[at, b * BS : (b + 1) * BS] = total.astype(jnp.bfloat16)

    res = res_ref[...]
    high = res.astype(jnp.bfloat16)
    rest = res - high.astype(jnp.float32)
    mid = rest.astype(jnp.bfloat16)
    low = (rest - mid.astype(jnp.float32)).astype(jnp.bfloat16)
    row = lax.broadcasted_iota(jnp.int32, (16, rows), 0)
    parts = jnp.where(
        row == 0,
        high.astype(jnp.float32),
        jnp.where(
            row == 1,
            mid.astype(jnp.float32),
            jnp.where(row == 2, low.astype(jnp.float32), 0.0),
        ),
    ).astype(jnp.bfloat16)
    base = panel_start(nblock, nblock)
    out_ref[base:, :] = jnp.zeros((out_ref.shape[0] - base, BS), jnp.float32)
    for b in range(nblock):
        part = mm(parts, design[:, b * BS : (b + 1) * BS], 1, 0, None)
        out_ref[base + b : base + b + 1, :] = jnp.sum(part, axis=0, keepdims=True) * scale

    @pl.loop(0, nsuper)
    def _(jj):
        right = design[:, pl.ds(pl.multiple_of(jj * SB, SB), SB)]
        first = pl.multiple_of(panel_start(nblock, 2 * jj), BS)
        second = pl.multiple_of(panel_start(nblock, 2 * jj + 1), BS)
        block = mm(right, right, 0, 0, None) * scale
        out_ref[pl.ds(first, SB), :] = block[:, :BS]
        out_ref[pl.ds(second, BS), :] = block[BS:, BS:]

        @pl.loop(jj + 1, nsuper)
        def _(ii):
            left = design[:, pl.ds(pl.multiple_of(ii * SB, SB), SB)]
            block = mm(left, right, 0, 0, None) * scale
            down = (ii - jj) * SB
            out_ref[pl.ds(pl.multiple_of(first + down, BS), SB), :] = block[:, :BS]
            out_ref[pl.ds(pl.multiple_of(second + down - BS, BS), SB), :] = block[:, BS:]


def factor_diag(a, e):
    sub = lax.broadcasted_iota(jnp.int32, (SUB, BS), 0)
    shape = (SUB, BS)
    count = BS // SUB

    def lane(x, j):
        return jnp.broadcast_to(x[:, j : j + 1], shape)

    def sublane(x, j):
        return jnp.broadcast_to(x[j : j + 1, :], shape)

    for p in range(count):
        base = p * SUB
        block = a[base : base + SUB, :]
        eblock = e[base : base + SUB, :]
        cols = [lane(block, base + j) for j in range(SUB)]
        scales, rows, erows, upper = [], [], [], {}
        for j in range(SUB):
            inv = lax.rsqrt(sublane(cols[j], j))
            scales.append(inv)
            mult = jnp.where(sub > j, cols[j] * inv, 0.0)
            for k in range(j + 1, SUB):
                upper[j, k] = sublane(cols[k], j) * inv
                cols[k] = cols[k] - mult * upper[j, k]
            row = sublane(block, j) * inv
            erow = sublane(eblock, j) * inv
            block = jnp.where(sub == j, row, block - mult * row)
            eblock = jnp.where(sub == j, erow, eblock - mult * erow)
            rows.append(row)
            erows.append(erow)
        a[base : base + SUB, :] = block
        e[base : base + SUB, :] = eblock
        for i in range(p + 1, count):
            at = slice(i * SUB, (i + 1) * SUB)
            below = a[at, :]
            ebelow = e[at, :]
            cols = [lane(below, base + j) for j in range(SUB)]
            for j in range(SUB):
                mult = cols[j] * scales[j]
                for k in range(j + 1, SUB):
                    cols[k] = cols[k] - mult * upper[j, k]
                below = below - mult * rows[j]
                ebelow = ebelow - mult * erows[j]
            a[at, :] = below
            e[at, :] = ebelow


def factor_kernel(nblock, place_ref, packed_ref, factor_ref, z_ref, w, inverse, a, e, y, sems):
    nsuper = nblock // 2
    size = nblock * BS
    base = panel_start(nblock, nblock)
    copies = []
    for k in range(nblock):
        begin = panel_start(nblock, k)
        copies.append(
            pltpu.make_async_copy(
                packed_ref.at[begin : begin + size - k * BS, :],
                w.at[k, k * BS : size, :],
                sems.at[k],
            )
        )
    copies.append(
        pltpu.make_async_copy(packed_ref.at[base : base + nblock, :], z_ref, sems.at[nblock])
    )
    for copy in copies:
        copy.start()
    for copy in copies:
        copy.wait()
    y[...] = jnp.zeros_like(y)
    for b in range(nblock):
        y[b // 2, 0:1, (b % 2) * BS : (b % 2 + 1) * BS] = z_ref[b : b + 1, :]
    row = lax.broadcasted_iota(jnp.int32, (BS, BS), 0)
    col = lax.broadcasted_iota(jnp.int32, (BS, BS), 1)
    eye = jnp.where(row == col, 1.0, 0.0).astype(jnp.float32)

    def wide(k, start, height):
        at = pl.ds(pl.multiple_of(start, BS), height)
        return jnp.concatenate([w[2 * k, at, :], w[2 * k + 1, at, :]], axis=1)

    @pl.loop(0, nsuper)
    def _(kk):
        top = pl.ds(pl.multiple_of(kk * SB, BS), BS)
        low = pl.ds(pl.multiple_of(kk * SB + BS, BS), BS)
        k = 2 * kk
        l21 = None
        e1 = None
        for half in range(2):
            if half == 0:
                a[...] = w[k, top, :]
            else:
                l21 = mm(w[k, low, :], e1, 1, 1)
                w[k, low, :] = l21
                a[...] = w[k + 1, low, :] - mm(l21, l21, 1, 1)
            e[...] = eye
            factor_diag(a, e)
            chol = jnp.where(row <= col, a[...], 0.0).T
            if half == 0:
                w[k, top, :] = chol
                e1 = jnp.where(row >= col, e[...], 0.0)
                inverse[kk, 0:BS, 0:BS] = e1
                inverse[kk, 0:BS, BS:SB] = jnp.zeros((BS, BS), jnp.float32)
            else:
                w[k + 1, low, :] = chol
                e2 = jnp.where(row >= col, e[...], 0.0)
                inverse[kk, BS:SB, BS:SB] = e2
                inverse[kk, BS:SB, 0:BS] = -mm(e2, mm(l21, e1, 1, 0), 1, 0)
        y[kk] = mm(y[kk], inverse[kk], 1, 1)

        @pl.loop(kk + 1, nsuper)
        def _(ii):
            at = pl.ds(pl.multiple_of(ii * SB, BS), SB)
            panel = mm3(wide(kk, ii * SB, SB), inverse[kk], 1, 1)
            w[k, at, :] = panel[:, :BS]
            w[k + 1, at, :] = panel[:, BS:]

        @pl.loop(kk + 1, nsuper)
        def _(jj):
            right = split(wide(kk, jj * SB, SB))
            y[jj] = y[jj] - mm3(y[kk], right, 1, 1)

            @pl.loop(jj, nsuper)
            def _(ii):
                at = pl.ds(pl.multiple_of(ii * SB, BS), SB)
                update = mm3(wide(kk, ii * SB, SB), right, 1, 1)
                w[2 * jj, at, :] = w[2 * jj, at, :] - update[:, :BS]
                w[2 * jj + 1, at, :] = w[2 * jj + 1, at, :] - update[:, BS:]

    @pl.loop(0, nsuper)
    def _(step):
        kk = nsuper - 1 - step

        def body(ii, total):
            return total - mm3(y[ii], wide(kk, ii * SB, SB), 1, 0)

        total = lax.fori_loop(kk + 1, nsuper, body, y[kk])
        y[kk] = mm(total, inverse[kk], 1, 0)

    for b in range(nblock):
        z_ref[b : b + 1, :] = y[b // 2, 0:1, (b % 2) * BS : (b % 2 + 1) * BS]

    per_row, per_col = factor_ref.shape[0], factor_ref.shape[2] // BS
    rows_of, cols_of = nblock // per_row, nblock // per_col
    for r in range(per_row):
        for c in range(per_col):
            rb = r * rows_of + place_ref[0]
            cb = c * cols_of + place_ref[1]
            block = w[cb, pl.ds(pl.multiple_of(rb * BS, BS), BS), :]
            keep = row + rb * BS >= col + cb * BS
            factor_ref[r, :, c * BS : (c + 1) * BS] = jnp.where(keep, block, 0.0)


UNIT = 2 * 6 * 8 * SUB
HALVE = 3


def exchange_kernel(chunks, term_ref, out_ref, acc, first, recv, sends, recvs):
    gx, gy, gz = lax.axis_index("gx"), lax.axis_index("gy"), lax.axis_index("gz")
    x, ylo = gx % 4, gx // 4
    z, core = gy // 2, gy % 2

    def flip(v):
        return v + 1 - 2 * (v % 2)

    def gray(v):
        return (v % 2) + (v // 2) - 2 * (v % 2) * (v // 2)

    y = 2 * gz + ylo
    ynext = 4 * (1 - ylo)
    partner = [
        {"gx": 4 * ylo + flip(x)},
        {"gx": ynext + x},
        {"gy": 2 * flip(z) + core},
        {"gx": 4 * ylo + 3 - x},
        {"gx": ynext + x, "gz": 1 - gz},
        {"gy": 2 * (3 - z) + core},
    ]
    bit = [gray(x), gray(y), gray(z), x // 2, y // 2, z // 2]
    mate = {"gy": 2 * z + 1 - core}
    rows = lambda at, size: pl.ds(pl.multiple_of(at, SUB), size)

    def remote(src, dst, c, s, p, device):
        return pltpu.make_async_remote_copy(
            src_ref=src,
            dst_ref=dst,
            send_sem=sends.at[c, s, p],
            recv_sem=recvs.at[c, s, p],
            device_id=device,
            device_id_type=pl.DeviceIdType.MESH,
        )

    def chunk(c):
        base, size = chunks[c]
        half, part = size // 2, size // 12
        pending = {}
        where = [0] * 6

        def stage(s):
            for p in range(6):
                local = base // 2 + p * part
                whole = base + core * half + p * part
                span = part >> min(s, HALVE)
                if s == 0:
                    other = base + (1 - core) * half + p * part
                    copy = remote(
                        term_ref.at[rows(other, part), :],
                        first.at[local : local + part, :],
                        c, 0, p, mate,
                    )
                    copy.start()
                    pending[0, p] = copy
                    continue
                pending[s - 1, p].wait_recv()
                if s == 1:
                    acc[local : local + part, :] = (
                        term_ref[rows(whole, part), :] + first[local : local + part, :]
                    )
                    span = part
                elif s <= 2 * HALVE + 1:
                    got = part >> min(s - 1, HALVE)
                    at = rows(local + where[p], got)
                    slot = slots[s - 1] + base // 12 // (part // got) * 6 + p * got
                    if s - 1 > HALVE:
                        pending[s - 1, p].wait_send()
                    total = acc[at, :] + recv[slot : slot + got, :]
                    if s <= 2 * HALVE:
                        acc[at, :] = total
                    else:
                        out_ref[rows(whole + where[p], got), :] = total
                    span = got
                if s <= HALVE:
                    g = (p + s - 1) % 6
                    span = part >> s
                    keep = where[p] + bit[g] * span
                    give = where[p] + (1 - bit[g]) * span
                    slot = slots[s] + base // 12 // (part // span) * 6 + p * span
                    copy = remote(
                        acc.at[rows(local + give, span), :],
                        recv.at[slot : slot + span, :],
                        c, s, p, partner[g],
                    )
                    where[p] = keep
                elif s <= 2 * HALVE:
                    g = (p + s - 1) % 6
                    slot = slots[s] + base // 12 // (part // span) * 6 + p * span
                    copy = remote(
                        acc.at[rows(local + where[p], span), :],
                        recv.at[slot : slot + span, :],
                        c, s, p, partner[g],
                    )
                elif s <= 3 * HALVE:
                    level = 3 * HALVE + 1 - s
                    g = (p + level - 1) % 6
                    span = part >> level
                    block = out_ref.at[rows(whole + where[p], span), :]
                    copy = remote(block, block, c, s, p, partner[g])
                    where[p] = where[p] - bit[g] * span
                elif s == 3 * HALVE + 1:
                    block = out_ref.at[rows(whole, part), :]
                    copy = remote(block, block, c, s, p, mate)
                else:
                    continue
                copy.start()
                pending[s, p] = copy

        def finish():
            for (s, p), copy in pending.items():
                if not HALVE < s <= 2 * HALVE:
                    copy.wait_send()

        return stage, finish

    slots, at = {}, 0
    total = sum(size for _, size in chunks) // 2
    for s in range(1, 2 * HALVE + 1):
        slots[s] = at
        at += total >> min(s, HALVE)
    runs = [chunk(c) for c in range(len(chunks))]
    last = 3 * HALVE + 2
    for t in range(last + len(chunks)):
        for c, (stage, _) in enumerate(runs):
            if 0 <= t - c <= last:
                stage(t - c)
    for _, finish in runs:
        finish()


def exchange(term, chunks):
    total, width = term.shape
    half = total // 2
    landing = sum(half >> min(s, HALVE) for s in range(1, 2 * HALVE + 1))
    vmem = pl.BlockSpec(memory_space=pltpu.VMEM)
    sem = pltpu.SemaphoreType.DMA((len(chunks), 3 * HALVE + 2, 6))
    return pl.pallas_call(
        functools.partial(exchange_kernel, chunks),
        out_shape=jax.ShapeDtypeStruct((total, width), jnp.float32),
        in_specs=[vmem],
        out_specs=vmem,
        scratch_shapes=[
            pltpu.VMEM((half, width), jnp.float32),
            pltpu.VMEM((half, width), jnp.float32),
            pltpu.VMEM((landing, width), jnp.float32),
            sem,
            sem,
        ],
        compiler_params=pltpu.CompilerParams(vmem_limit_bytes=VMEM_LIMIT, has_side_effects=True),
    )(term)


def on_device(blocks, coefficients, residuals):
    row_count = lax.axis_size("gx")
    col_count = lax.axis_size("gy")
    devices = row_count * col_count * lax.axis_size("gz")
    rows, slots, width = coefficients.shape
    scale = 1.0 / (rows * devices)
    nblock = G // width
    nsuper = nblock // 2
    used = panel_start(nblock, nblock) + nblock
    units = -(-used // UNIT)
    counts = [units // 3 + (i < units % 3) for i in range(3)]
    chunks = [(UNIT * sum(counts[:i]), UNIT * counts[i]) for i in range(3)]
    total = UNIT * units
    vmem = pl.BlockSpec(memory_space=pltpu.VMEM)
    term = pl.pallas_call(
        functools.partial(gram_kernel, nblock, scale),
        out_shape=jax.ShapeDtypeStruct((total, width), jnp.float32),
        in_specs=[vmem] * 3,
        out_specs=vmem,
        scratch_shapes=[pltpu.VMEM((rows, G), jnp.bfloat16)],
        compiler_params=pltpu.CompilerParams(vmem_limit_bytes=VMEM_LIMIT),
    )(blocks, coefficients.transpose(1, 0, 2), residuals.reshape(1, rows))
    packed = exchange(term, chunks)
    place = jnp.stack([lax.axis_index("gx"), lax.axis_index("gy")]).astype(jnp.int32)
    per_row, per_col = nblock // row_count, nblock // col_count
    factor, answer = pl.pallas_call(
        functools.partial(factor_kernel, nblock),
        out_shape=(
            jax.ShapeDtypeStruct((per_row, width, per_col * width), jnp.float32),
            jax.ShapeDtypeStruct((nblock, width), jnp.float32),
        ),
        in_specs=[pl.BlockSpec(memory_space=pltpu.SMEM), pl.BlockSpec(memory_space=pl.ANY)],
        out_specs=(vmem, vmem),
        scratch_shapes=[
            pltpu.VMEM((nblock, G, width), jnp.float32),
            pltpu.VMEM((nsuper, SB, SB), jnp.float32),
            pltpu.VMEM((width, width), jnp.float32),
            pltpu.VMEM((width, width), jnp.float32),
            pltpu.VMEM((nsuper, SUB, SB), jnp.float32),
            pltpu.SemaphoreType.DMA((nblock + 1,)),
        ],
        compiler_params=pltpu.CompilerParams(vmem_limit_bytes=VMEM_LIMIT),
    )(place, packed)
    return (factor.reshape(1, per_row, width, 1, per_col, width), answer)


def solution(mesh):
    in_specs = (
        P(("gx", "gy", "gz"), None),
        P(("gx", "gy", "gz"), None, None),
        P(("gx", "gy", "gz")),
    )
    out_specs = (P("gx", None, None, "gy", None, None), P())
    return jax.shard_map(
        on_device, mesh=mesh, in_specs=in_specs, out_specs=out_specs, check_vma=False
    )
```

```python
import functools

import jax
import jax.numpy as jnp
from jax import lax
from jax.experimental import pallas as pl
from jax.experimental.pallas import tpu as pltpu
from jax.sharding import PartitionSpec as P

G = 2048
BS = 128
SB = 2 * BS
SUB = 8
HB = BS // 2
VMEM_LIMIT = 60 * 1024 * 1024


def mm(a, b, ca, cb, precision=lax.Precision.HIGHEST):
    return lax.dot_general(
        a, b, (((ca,), (cb,)), ((), ())), precision=precision, preferred_element_type=jnp.float32
    )

def split(x):
    high = x.astype(jnp.bfloat16)
    return high, (x - high.astype(jnp.float32)).astype(jnp.bfloat16)

def mm3(a, b, ca, cb):
    ah, al = a if isinstance(a, tuple) else split(a)
    bh, bl = b if isinstance(b, tuple) else split(b)
    return mm(
        jnp.concatenate([ah, ah, al], axis=ca), jnp.concatenate([bh, bl, bh], axis=cb), ca, cb, None
    )

def panel_start(nblock, k):
    return BS * (nblock * k - (k * (k - 1)) // 2)

def chol_half(x, off, fill):
    shape = (SUB, BS)
    sub = lax.broadcasted_iota(jnp.int32, shape, 0)
    count = len(x)
    x = list(x)

    def lane(v, j):
        return jnp.broadcast_to(v[:, off + j : off + j + 1], shape)

    def sublane(v, j):
        return jnp.broadcast_to(v[j : j + 1, :], shape)

    def lanes(v, p):
        return [lane(v, p * SUB + j) for j in range(SUB)]

    cols = lanes(x[0], 0)
    ahead = lanes(x[1], 1)
    below = {i: lanes(x[i], 0) for i in range(1, count)}
    for p in range(count):
        if p % 2 == 1:
            fill()
        block = x[p]
        scales, rows, upper = [], [], {}
        for j in range(SUB):
            inv = lax.rsqrt(sublane(cols[j], j))
            mult = jnp.where(sub > j, cols[j] * inv, 0.0)
            for k in range(j + 1, SUB):
                upper[j, k] = sublane(cols[k], j) * inv
                cols[k] = cols[k] - mult * upper[j, k]
            row = sublane(block, j) * inv
            block = jnp.where(sub == j, row, block - mult * row)
            scales.append(inv)
            rows.append(row)
        x[p] = block
        fresh, reach = {}, None
        for i in range(p + 1, count):
            b = below[i]
            mults = []
            for j in range(SUB):
                m = b[j] * scales[j]
                mults.append(m)
                for k in range(j + 1, SUB):
                    b[k] = b[k] - m * upper[j, k]
            if i == p + 1:
                for k in range(SUB):
                    for j in range(SUB):
                        ahead[k] = ahead[k] - mults[j] * sublane(mults[j], k)
            for j in range(SUB):
                x[i] = x[i] - mults[j] * rows[j]
            if i > p + 1:
                fresh[i] = lanes(x[i], p + 1)
                if i == p + 2:
                    reach = lanes(x[i], p + 2)
        cols, ahead, below = ahead, reach, fresh
    return x

def chol_block(t, fill=lambda: None):
    row = lax.broadcasted_iota(jnp.int32, (BS, BS), 0)
    col = lax.broadcasted_iota(jnp.int32, (BS, BS), 1)
    hrow, hcol = row[:HB], col[:HB]

    def rowsof(v):
        return [v[i * SUB : (i + 1) * SUB, :] for i in range(HB // SUB)]

    zero = jnp.zeros((HB, BS), jnp.float32)
    top = t[:HB]
    first = jnp.where(hcol < HB, top, jnp.where(hcol - HB == hrow, 1.0, 0.0))
    xa = jnp.concatenate(chol_half(rowsof(first), 0, fill), axis=0)
    ea = jnp.where((hcol >= HB) & (hcol - HB <= hrow), xa, 0.0)
    ua = mm3(ea, jnp.concatenate([zero, top], axis=0), 1, 0)
    u12 = split(jnp.where(hcol >= HB, ua, 0.0))
    low = t[HB:] - mm3(u12, u12, 0, 0)[HB:]
    second = jnp.where(hcol >= HB, low, jnp.where(hcol == hrow, 1.0, 0.0))
    xb = jnp.concatenate(chol_half(rowsof(second), HB, fill), axis=0)
    eb = jnp.where(hcol <= hrow, xb, 0.0)
    w = mm3(u12, ea, 0, 0)[HB:]
    e21 = mm3(eb, jnp.concatenate([w, zero], axis=0), 1, 0)
    lowrow = jnp.where(hcol < HB, eb, -e21)
    inverse = pltpu.roll(jnp.concatenate([ea, lowrow], axis=0), HB, 1)
    upper = jnp.concatenate([jnp.where(hcol < HB, jnp.where(hrow <= hcol, xa, 0.0), ua),
                             jnp.where(hcol - HB >= hrow, xb, 0.0)], axis=0)
    return upper.T, inverse

def factor_body(nblock, place_ref, packed_ref, factor_ref, z_ref, wh, wl, tiles, y, inv_h, inv_l, arrive=None):
    nsuper = nblock // 2
    base = panel_start(nblock, nblock)

    def at(ii):
        return pl.ds(pl.multiple_of(ii * SB, SB), SB)

    def both(j, ii):
        return wh[j, at(ii), :], wl[j, at(ii), :]

    def fetch(kk):
        first = BS * ((2 * nblock + 1) * kk - 2 * kk * kk)
        second = first + BS * (nblock - 2 * kk) - BS

        @pl.loop(kk, nsuper)
        def _(ii):
            for side, begin in enumerate((first, second)):
                rows = pl.ds(pl.multiple_of(begin + (ii - kk) * SB, BS), SB)
                tiles[kk % 2, at(ii), side * BS : (side + 1) * BS] = packed_ref[rows, :]

    for b in range(nblock):
        y[b // 2, 0:1, (b % 2) * BS : (b % 2 + 1) * BS] = packed_ref[base + b : base + b + 1, :]
        if b % 2 == 0:
            y[b // 2, 1:SUB, :] = jnp.zeros((SUB - 1, SB), jnp.float32)
    row = lax.broadcasted_iota(jnp.int32, (BS, BS), 0)
    col = lax.broadcasted_iota(jnp.int32, (BS, BS), 1)
    zero = jnp.zeros((BS, BS), jnp.float32)
    wh[0, 0:SB, :] = jnp.zeros((SB, SB), jnp.bfloat16)
    wl[0, 0:SB, :] = jnp.zeros((SB, SB), jnp.bfloat16)
    tiles[0, nsuper * SB :, :] = jnp.zeros((SB, SB), jnp.float32)
    fetch(0)
    fetch(1)

    @pl.loop(0, nsuper)
    def _(kk):
        last = jnp.maximum(kk - 1, 0)
        here, there = kk % 2, (kk + 1) % 2
        rest = nsuper - 1 - kk
        cursor = [kk + 1, 0]

        def filler(n):
            first = n < rest
            ii2, j2 = cursor
            some = (kk > 0) & (ii2 < nsuper)
            valid = jnp.where(first, kk > 0, some)
            j = jnp.where(valid, jnp.where(first, last, j2), 0)
            ii = jnp.where(valid, jnp.where(first, kk + 1 + n, ii2), 0)
            other = jnp.where(valid, jnp.where(first, kk, kk + 1), 0)
            spot = jnp.where(valid, jnp.where(first, here, there), 0)
            dest = jnp.where(valid, ii, nsuper)
            moved = jnp.where(first, j2, j2 + 1)
            done = jnp.logical_not(first) & (moved >= kk)
            cursor[0] = jnp.where(done, ii2 + 1, ii2)
            cursor[1] = jnp.where(done, 0, moved)
            tiles[spot, at(dest), :] = tiles[spot, at(dest), :] - mm3(both(j, ii), both(j, other), 1, 1)

        diag = tiles[here, at(kk), :]
        steps = iter(range(16))

        def fill():
            n = next(steps, None)
            if n is not None:
                filler(n)

        ykk = y[kk] - jnp.where(kk > 0, mm3(y[last], both(last, kk), 1, 1), 0.0)
        la, ea = chol_block(diag[0:BS, 0:BS], fill)
        eas = split(ea)
        l21 = mm3(diag[BS:SB, 0:BS], eas, 1, 1)
        l21s = split(l21)
        lb, eb = chol_block(diag[BS:SB, BS:SB] - mm3(l21s, l21s, 1, 1), fill)
        ec = -mm3(eb, mm3(l21s, eas, 1, 0), 1, 0)
        inv = split(jnp.concatenate(
            [jnp.concatenate([ea, zero], axis=1), jnp.concatenate([ec, eb], axis=1)], axis=0))
        low = jnp.concatenate(
            [jnp.concatenate([la, zero], axis=1), jnp.concatenate([l21, lb], axis=1)], axis=0)
        wh[kk, at(kk), :], wl[kk, at(kk), :] = split(low)
        inv_h[kk], inv_l[kk] = inv
        y[kk] = mm3(ykk, inv, 1, 1)

        @pl.loop(kk + 1, nsuper)
        def _(ii):
            y[ii] = y[ii] - jnp.where(kk > 0, mm3(y[last], both(last, ii), 1, 1), 0.0)
            wh[kk, at(ii), :], wl[kk, at(ii), :] = split(
                mm3(tiles[here, at(ii), :], (inv_h[kk], inv_l[kk]), 1, 1))

        @pl.when(kk + 1 < nsuper)
        def _():
            side = both(kk, kk + 1)
            tiles[there, at(kk + 1), :] = tiles[there, at(kk + 1), :] - mm3(side, side, 1, 1)

        @pl.when(kk + 2 < nsuper)
        def _():
            fetch(kk + 2)

    @pl.loop(0, nsuper)
    def _(step):
        kk = nsuper - 1 - step
        y[kk] = mm3(y[kk], (inv_h[kk], inv_l[kk]), 1, 0)
        x = split(y[kk])

        @pl.loop(0, kk)
        def _(j):
            y[j] = y[j] - mm3(x, both(j, kk), 1, 0)

    for b in range(nblock):
        z_ref[b : b + 1, :] = y[b // 2, 0:1, (b % 2) * BS : (b % 2 + 1) * BS]

    per_row, per_col = factor_ref.shape[0], factor_ref.shape[2] // BS
    rows_of, cols_of = nblock // per_row, nblock // per_col
    for r in range(per_row):
        for c in range(per_col):
            rb = r * rows_of + place_ref[0]
            cb = c * cols_of + place_ref[1]
            rows = pl.ds(pl.multiple_of(rb * BS, BS), BS)
            wide = wh[cb // 2, rows, :].astype(jnp.float32) + wl[cb // 2, rows, :].astype(jnp.float32)
            block = jnp.where(cb % 2 == 0, wide[:, :BS], wide[:, BS:])
            keep = row + rb * BS >= col + cb * BS
            factor_ref[r, :, c * BS : (c + 1) * BS] = jnp.where(keep, block, 0.0)

def factor_kernel(*args):
    factor_body(*args)

def gram_kernel(nblock, scale, blocks_ref, coef_ref, res_ref, out_ref, design):
    slots = coef_ref.shape[0]
    rows = coef_ref.shape[1]
    chunk = 128
    nsuper = nblock // 2

    @pl.loop(0, rows // chunk)
    def _(t):
        at = pl.ds(pl.multiple_of(t * chunk, chunk), chunk)
        idx = blocks_ref[at, :]
        labels = [jnp.broadcast_to(idx[:, s : s + 1], (chunk, BS)) for s in range(slots)]
        values = [coef_ref[s, at, :].astype(jnp.float32) for s in range(slots)]
        for b in range(nblock):
            total = jnp.where(labels[0] == b, values[0], 0.0)
            for s in range(1, slots):
                total = jnp.where(labels[s] == b, values[s], total)
            design[at, b * BS : (b + 1) * BS] = total.astype(jnp.bfloat16)

    res = res_ref[...]
    high = res.astype(jnp.bfloat16)
    rest = res - high.astype(jnp.float32)
    mid = rest.astype(jnp.bfloat16)
    low = (rest - mid.astype(jnp.float32)).astype(jnp.bfloat16)
    row = lax.broadcasted_iota(jnp.int32, (16, rows), 0)
    parts = jnp.where(
        row == 0,
        high.astype(jnp.float32),
        jnp.where(
            row == 1,
            mid.astype(jnp.float32),
            jnp.where(row == 2, low.astype(jnp.float32), 0.0),
        ),
    ).astype(jnp.bfloat16)
    base = panel_start(nblock, nblock)
    out_ref[base:, :] = jnp.zeros((out_ref.shape[0] - base, BS), jnp.float32)
    for b in range(nblock):
        part = mm(parts, design[:, b * BS : (b + 1) * BS], 1, 0, None)
        out_ref[base + b : base + b + 1, :] = jnp.sum(part, axis=0, keepdims=True) * scale

    @pl.loop(0, nsuper)
    def _(jj):
        right = design[:, pl.ds(pl.multiple_of(jj * SB, SB), SB)]
        first = pl.multiple_of(panel_start(nblock, 2 * jj), BS)
        second = pl.multiple_of(panel_start(nblock, 2 * jj + 1), BS)
        block = mm(right, right, 0, 0, None) * scale
        out_ref[pl.ds(first, SB), :] = block[:, :BS]
        out_ref[pl.ds(second, BS), :] = block[BS:, BS:]

        @pl.loop(jj + 1, nsuper)
        def _(ii):
            left = design[:, pl.ds(pl.multiple_of(ii * SB, SB), SB)]
            block = mm(left, right, 0, 0, None) * scale
            down = (ii - jj) * SB
            out_ref[pl.ds(pl.multiple_of(first + down, BS), SB), :] = block[:, :BS]
            out_ref[pl.ds(pl.multiple_of(second + down - BS, BS), SB), :] = block[:, BS:]


UNIT = 2 * 6 * 8 * SUB
HALVE = 3


def exchange_kernel(chunks, term_ref, out_ref, acc, first, recv, sends, recvs):
    gx, gy, gz = lax.axis_index("gx"), lax.axis_index("gy"), lax.axis_index("gz")
    x, ylo = gx % 4, gx // 4
    z, core = gy // 2, gy % 2

    def flip(v):
        return v + 1 - 2 * (v % 2)

    def gray(v):
        return (v % 2) + (v // 2) - 2 * (v % 2) * (v // 2)

    y = 2 * gz + ylo
    ynext = 4 * (1 - ylo)
    partner = [
        {"gx": 4 * ylo + flip(x)},
        {"gx": ynext + x},
        {"gy": 2 * flip(z) + core},
        {"gx": 4 * ylo + 3 - x},
        {"gx": ynext + x, "gz": 1 - gz},
        {"gy": 2 * (3 - z) + core},
    ]
    bit = [gray(x), gray(y), gray(z), x // 2, y // 2, z // 2]
    mate = {"gy": 2 * z + 1 - core}
    rows = lambda at, size: pl.ds(pl.multiple_of(at, SUB), size)

    def remote(src, dst, c, s, p, device):
        return pltpu.make_async_remote_copy(
            src_ref=src,
            dst_ref=dst,
            send_sem=sends.at[c, s, p],
            recv_sem=recvs.at[c, s, p],
            device_id=device,
            device_id_type=pl.DeviceIdType.MESH,
        )

    def chunk(c):
        base, size = chunks[c]
        half, part = size // 2, size // 12
        pending = {}
        where = [0] * 6

        def stage(s):
            for p in range(6):
                local = base // 2 + p * part
                whole = base + core * half + p * part
                span = part >> min(s, HALVE)
                if s == 0:
                    other = base + (1 - core) * half + p * part
                    copy = remote(
                        term_ref.at[rows(other, part), :],
                        first.at[local : local + part, :],
                        c, 0, p, mate,
                    )
                    copy.start()
                    pending[0, p] = copy
                    continue
                pending[s - 1, p].wait_recv()
                if s == 1:
                    acc[local : local + part, :] = (
                        term_ref[rows(whole, part), :] + first[local : local + part, :]
                    )
                    span = part
                elif s <= 2 * HALVE + 1:
                    got = part >> min(s - 1, HALVE)
                    at = rows(local + where[p], got)
                    slot = slots[s - 1] + base // 12 // (part // got) * 6 + p * got
                    if s - 1 > HALVE:
                        pending[s - 1, p].wait_send()
                    total = acc[at, :] + recv[slot : slot + got, :]
                    if s <= 2 * HALVE:
                        acc[at, :] = total
                    else:
                        out_ref[rows(whole + where[p], got), :] = total
                    span = got
                if s <= HALVE:
                    g = (p + s - 1) % 6
                    span = part >> s
                    keep = where[p] + bit[g] * span
                    give = where[p] + (1 - bit[g]) * span
                    slot = slots[s] + base // 12 // (part // span) * 6 + p * span
                    copy = remote(
                        acc.at[rows(local + give, span), :],
                        recv.at[slot : slot + span, :],
                        c, s, p, partner[g],
                    )
                    where[p] = keep
                elif s <= 2 * HALVE:
                    g = (p + s - 1) % 6
                    slot = slots[s] + base // 12 // (part // span) * 6 + p * span
                    copy = remote(
                        acc.at[rows(local + where[p], span), :],
                        recv.at[slot : slot + span, :],
                        c, s, p, partner[g],
                    )
                elif s <= 3 * HALVE:
                    level = 3 * HALVE + 1 - s
                    g = (p + level - 1) % 6
                    span = part >> level
                    block = out_ref.at[rows(whole + where[p], span), :]
                    copy = remote(block, block, c, s, p, partner[g])
                    where[p] = where[p] - bit[g] * span
                elif s == 3 * HALVE + 1:
                    block = out_ref.at[rows(whole, part), :]
                    copy = remote(block, block, c, s, p, mate)
                else:
                    continue
                copy.start()
                pending[s, p] = copy

        def finish():
            for (s, p), copy in pending.items():
                if not HALVE < s <= 2 * HALVE:
                    copy.wait_send()

        return stage, finish

    slots, at = {}, 0
    total = sum(size for _, size in chunks) // 2
    for s in range(1, 2 * HALVE + 1):
        slots[s] = at
        at += total >> min(s, HALVE)
    runs = [chunk(c) for c in range(len(chunks))]
    last = 3 * HALVE + 2
    for t in range(last + len(chunks)):
        for c, (stage, _) in enumerate(runs):
            if 0 <= t - c <= last:
                stage(t - c)
    for _, finish in runs:
        finish()


def exchange(term, chunks):
    total, width = term.shape
    half = total // 2
    landing = sum(half >> min(s, HALVE) for s in range(1, 2 * HALVE + 1))
    vmem = pl.BlockSpec(memory_space=pltpu.VMEM)
    sem = pltpu.SemaphoreType.DMA((len(chunks), 3 * HALVE + 2, 6))
    return pl.pallas_call(
        functools.partial(exchange_kernel, chunks),
        out_shape=jax.ShapeDtypeStruct((total, width), jnp.float32),
        in_specs=[vmem],
        out_specs=vmem,
        scratch_shapes=[
            pltpu.VMEM((half, width), jnp.float32),
            pltpu.VMEM((half, width), jnp.float32),
            pltpu.VMEM((landing, width), jnp.float32),
            sem,
            sem,
        ],
        compiler_params=pltpu.CompilerParams(vmem_limit_bytes=VMEM_LIMIT, has_side_effects=True),
    )(term)


def on_device(blocks, coefficients, residuals):
    row_count = lax.axis_size("gx")
    col_count = lax.axis_size("gy")
    devices = row_count * col_count * lax.axis_size("gz")
    rows, slots, width = coefficients.shape
    scale = 1.0 / (rows * devices)
    nblock = G // width
    nsuper = nblock // 2
    used = panel_start(nblock, nblock) + nblock
    units = -(-used // UNIT)
    counts = [units // 3 + (i < units % 3) for i in range(3)]
    chunks = [(UNIT * sum(counts[:i]), UNIT * counts[i]) for i in range(3)]
    total = UNIT * units
    vmem = pl.BlockSpec(memory_space=pltpu.VMEM)
    term = pl.pallas_call(
        functools.partial(gram_kernel, nblock, scale),
        out_shape=jax.ShapeDtypeStruct((total, width), jnp.float32),
        in_specs=[vmem] * 3,
        out_specs=vmem,
        scratch_shapes=[pltpu.VMEM((rows, G), jnp.bfloat16)],
        compiler_params=pltpu.CompilerParams(vmem_limit_bytes=VMEM_LIMIT),
    )(blocks, coefficients.transpose(1, 0, 2), residuals.reshape(1, rows))
    packed = exchange(term, chunks)
    place = jnp.stack([lax.axis_index("gx"), lax.axis_index("gy")]).astype(jnp.int32)
    per_row, per_col = nblock // row_count, nblock // col_count
    factor, answer = pl.pallas_call(
        functools.partial(factor_kernel, nblock),
        out_shape=(
            jax.ShapeDtypeStruct((per_row, width, per_col * width), jnp.float32),
            jax.ShapeDtypeStruct((nblock, width), jnp.float32),
        ),
        in_specs=[pl.BlockSpec(memory_space=pltpu.SMEM), vmem],
        out_specs=(vmem, vmem),
        scratch_shapes=[
            pltpu.VMEM((nsuper, G, SB), jnp.bfloat16),
            pltpu.VMEM((nsuper, G, SB), jnp.bfloat16),
            pltpu.VMEM((2, G + SB, SB), jnp.float32),
            pltpu.VMEM((nsuper, SUB, SB), jnp.float32),
            pltpu.VMEM((nsuper, SB, SB), jnp.bfloat16),
            pltpu.VMEM((nsuper, SB, SB), jnp.bfloat16),
        ],
        compiler_params=pltpu.CompilerParams(vmem_limit_bytes=VMEM_LIMIT),
    )(place, packed)
    return (factor.reshape(1, per_row, width, 1, per_col, width), answer)


def solution(mesh):
    in_specs = (
        P(("gx", "gy", "gz"), None),
        P(("gx", "gy", "gz"), None, None),
        P(("gx", "gy", "gz")),
    )
    out_specs = (P("gx", None, None, "gy", None, None), P())
    return jax.shard_map(
        on_device, mesh=mesh, in_specs=in_specs, out_specs=out_specs, check_vma=False
    )
```

```python
import functools

import jax
import jax.numpy as jnp
from jax import lax
from jax.experimental import pallas as pl
from jax.experimental.pallas import tpu as pltpu
from jax.sharding import PartitionSpec as P

G = 2048
BS = 128
SB = 2 * BS
SUB = 8
HB = BS // 2
VMEM_LIMIT = 63 * 1024 * 1024
UNIT = 2 * 6 * 8 * SUB
HALVE = 3


def mm(a, b, ca, cb, precision=lax.Precision.HIGHEST):
    return lax.dot_general(
        a, b, (((ca,), (cb,)), ((), ())), precision=precision, preferred_element_type=jnp.float32
    )

def split(x):
    high = x.astype(jnp.bfloat16)
    return high, (x - high.astype(jnp.float32)).astype(jnp.bfloat16)

def mm3(a, b, ca, cb):
    ah, al = a if isinstance(a, tuple) else split(a)
    bh, bl = b if isinstance(b, tuple) else split(b)
    return mm(
        jnp.concatenate([ah, ah, al], axis=ca), jnp.concatenate([bh, bl, bh], axis=cb), ca, cb, None
    )

def panel_start(nblock, k):
    return BS * (nblock * k - (k * (k - 1)) // 2)

def chol_half(x, off, fill):
    shape = (SUB, BS)
    sub = lax.broadcasted_iota(jnp.int32, shape, 0)
    count = len(x)
    x = list(x)

    def lane(v, j):
        return jnp.broadcast_to(v[:, off + j : off + j + 1], shape)

    def sublane(v, j):
        return jnp.broadcast_to(v[j : j + 1, :], shape)

    def lanes(v, p):
        return [lane(v, p * SUB + j) for j in range(SUB)]

    cols = lanes(x[0], 0)
    ahead = lanes(x[1], 1)
    below = {i: lanes(x[i], 0) for i in range(1, count)}
    for p in range(count):
        if p % 2 == 1:
            fill()
        block = x[p]
        scales, rows, upper = [], [], {}
        for j in range(SUB):
            inv = lax.rsqrt(sublane(cols[j], j))
            mult = jnp.where(sub > j, cols[j] * inv, 0.0)
            for k in range(j + 1, SUB):
                upper[j, k] = sublane(cols[k], j) * inv
                cols[k] = cols[k] - mult * upper[j, k]
            row = sublane(block, j) * inv
            block = jnp.where(sub == j, row, block - mult * row)
            scales.append(inv)
            rows.append(row)
        x[p] = block
        fresh, reach = {}, None
        for i in range(p + 1, count):
            b = below[i]
            mults = []
            for j in range(SUB):
                m = b[j] * scales[j]
                mults.append(m)
                for k in range(j + 1, SUB):
                    b[k] = b[k] - m * upper[j, k]
            if i == p + 1:
                for k in range(SUB):
                    for j in range(SUB):
                        ahead[k] = ahead[k] - mults[j] * sublane(mults[j], k)
            for j in range(SUB):
                x[i] = x[i] - mults[j] * rows[j]
            if i > p + 1:
                fresh[i] = lanes(x[i], p + 1)
                if i == p + 2:
                    reach = lanes(x[i], p + 2)
        cols, ahead, below = ahead, reach, fresh
    return x

def chol_block(t, fill=lambda: None):
    row = lax.broadcasted_iota(jnp.int32, (BS, BS), 0)
    col = lax.broadcasted_iota(jnp.int32, (BS, BS), 1)
    hrow, hcol = row[:HB], col[:HB]

    def rowsof(v):
        return [v[i * SUB : (i + 1) * SUB, :] for i in range(HB // SUB)]

    zero = jnp.zeros((HB, BS), jnp.float32)
    top = t[:HB]
    first = jnp.where(hcol < HB, top, jnp.where(hcol - HB == hrow, 1.0, 0.0))
    xa = jnp.concatenate(chol_half(rowsof(first), 0, fill), axis=0)
    ea = jnp.where((hcol >= HB) & (hcol - HB <= hrow), xa, 0.0)
    ua = mm3(ea, jnp.concatenate([zero, top], axis=0), 1, 0)
    u12 = split(jnp.where(hcol >= HB, ua, 0.0))
    low = t[HB:] - mm3(u12, u12, 0, 0)[HB:]
    second = jnp.where(hcol >= HB, low, jnp.where(hcol == hrow, 1.0, 0.0))
    xb = jnp.concatenate(chol_half(rowsof(second), HB, fill), axis=0)
    eb = jnp.where(hcol <= hrow, xb, 0.0)
    w = mm3(u12, ea, 0, 0)[HB:]
    e21 = mm3(eb, jnp.concatenate([w, zero], axis=0), 1, 0)
    lowrow = jnp.where(hcol < HB, eb, -e21)
    inverse = pltpu.roll(jnp.concatenate([ea, lowrow], axis=0), HB, 1)
    upper = jnp.concatenate([jnp.where(hcol < HB, jnp.where(hrow <= hcol, xa, 0.0), ua),
                             jnp.where(hcol - HB >= hrow, xb, 0.0)], axis=0)
    return upper.T, inverse

def layout(nblock):
    nsuper = nblock // 2
    sizes = [BS * (2 * nblock - 4 * j - 1) for j in range(nsuper)]
    begins, chunks, at = {}, [], 0
    for group in ((0, nsuper - 1), (1, 2), range(3, nsuper - 1)):
        base = at
        for j in group:
            begins[j] = at
            at += sizes[j]
        if base == 0:
            rhs = at
            at += nblock
        used = at
        at = base + -(-(at - base) // UNIT) * UNIT
        chunks.append((base, at - base, used))
    return begins, rhs, chunks, at


def factor_all(nblock, begins, rhs, packed, factor_ref, z_ref, wh, wl, tiles, y, inv_h, inv_l, hooks):
    nsuper = nblock // 2

    def at(ii):
        return pl.ds(pl.multiple_of(ii * SB, SB), SB)

    def spot(j, ii):
        return (j * (2 * nsuper + 1 - j)) // 2 + ii - j

    def both(j, ii):
        k = spot(j, ii)
        return wh[k], wl[k]

    def keep(j, ii, value):
        k = spot(j, ii)
        wh[k], wl[k] = split(value)

    def fetch(kk):
        if isinstance(kk, int):
            first = begins[kk]
        else:
            first = jnp.int32(begins[0])
            for j in range(1, nsuper):
                first = jnp.where(kk == j, begins[j], first)
        second = first + BS * (nblock - 2 * kk) - BS

        @pl.loop(kk, nsuper)
        def _(ii):
            for side, begin in enumerate((first, second)):
                rows = pl.ds(pl.multiple_of(begin + (ii - kk) * SB, BS), SB)
                tiles[kk % 2, at(ii), side * BS : (side + 1) * BS] = packed[rows, :]

    row = lax.broadcasted_iota(jnp.int32, (BS, BS), 0)
    col = lax.broadcasted_iota(jnp.int32, (BS, BS), 1)
    zero = jnp.zeros((BS, BS), jnp.float32)
    tiles[0, nsuper * SB :, :] = jnp.zeros((SB, SB), jnp.float32)
    for b in range(nblock):
        y[b // 2, 0:1, (b % 2) * BS : (b % 2 + 1) * BS] = packed[rhs + b : rhs + b + 1, :]
        if b % 2 == 0:
            y[b // 2, 1:SUB, :] = jnp.zeros((SUB - 1, SB), jnp.float32)
    fetch(0)

    def pivot(kk, here, ykk, fill):
        diag = tiles[here, at(kk), :]
        la, ea = chol_block(diag[0:BS, 0:BS], fill)
        eas = split(ea)
        l21 = mm3(diag[BS:SB, 0:BS], eas, 1, 1)
        l21s = split(l21)
        lb, eb = chol_block(diag[BS:SB, BS:SB] - mm3(l21s, l21s, 1, 1), fill)
        ec = -mm3(eb, mm3(l21s, eas, 1, 0), 1, 0)
        inv = split(jnp.concatenate(
            [jnp.concatenate([ea, zero], axis=1), jnp.concatenate([ec, eb], axis=1)], axis=0))
        low = jnp.concatenate(
            [jnp.concatenate([la, zero], axis=1), jnp.concatenate([l21, lb], axis=1)], axis=0)
        keep(kk, kk, low)
        inv_h[kk], inv_l[kk] = inv
        y[kk] = mm3(ykk, inv, 1, 1)

    def solve(kk, here, ii):
        keep(kk, ii, mm3(tiles[here, at(ii), :], (inv_h[kk], inv_l[kk]), 1, 1))

    def onward(kk, there):
        side = both(kk, kk + 1)
        tiles[there, at(kk + 1), :] = tiles[there, at(kk + 1), :] - mm3(side, side, 1, 1)

    early = iter(range(2 * SUB))
    pivot(0, 0, y[0], lambda: hooks["pivot"](next(early)))

    @pl.loop(1, nsuper)
    def _(ii):
        solve(0, 0, ii)

    hooks["solved"]()
    fetch(1)
    onward(0, 1)
    fetch(2)

    @pl.loop(1, nsuper)
    def _(kk):
        last = kk - 1
        here, there = kk % 2, (kk + 1) % 2
        rest = nsuper - 1 - kk
        cursor = [kk + 1, 0]

        def filler(n):
            first = n < rest
            ii2, j2 = cursor
            valid = first | (ii2 < nsuper)
            j = jnp.where(valid, jnp.where(first, last, j2), 0)
            ii = jnp.where(valid, jnp.where(first, kk + 1 + n, ii2), 0)
            other = jnp.where(valid, jnp.where(first, kk, kk + 1), 0)
            side = jnp.where(valid, jnp.where(first, here, there), 0)
            dest = jnp.where(valid, ii, nsuper)
            moved = jnp.where(first, j2, j2 + 1)
            done = jnp.logical_not(first) & (moved >= kk)
            cursor[0] = jnp.where(done, ii2 + 1, ii2)
            cursor[1] = jnp.where(done, 0, moved)
            tiles[side, at(dest), :] = tiles[side, at(dest), :] - mm3(both(j, ii), both(j, other), 1, 1)

        steps = iter(range(2 * SUB))
        ykk = y[kk] - mm3(y[last], both(last, kk), 1, 1)
        pivot(kk, here, ykk, lambda: filler(next(steps)))

        @pl.loop(kk + 1, nsuper)
        def _(ii):
            y[ii] = y[ii] - mm3(y[last], both(last, ii), 1, 1)
            solve(kk, here, ii)

        @pl.when(kk + 1 < nsuper)
        def _():
            onward(kk, there)

        @pl.when(kk == 1)
        def _():
            hooks["second"]()

        @pl.when(kk + 2 < nsuper)
        def _():
            fetch(kk + 2)

    @pl.loop(0, nsuper)
    def _(step):
        kk = nsuper - 1 - step
        y[kk] = mm3(y[kk], (inv_h[kk], inv_l[kk]), 1, 0)
        x = split(y[kk])

        @pl.loop(0, kk)
        def _(j):
            y[j] = y[j] - mm3(x, both(j, kk), 1, 0)

    for b in range(nblock):
        z_ref[b : b + 1, :] = y[b // 2, 0:1, (b % 2) * BS : (b % 2 + 1) * BS]

    per_row, per_col = factor_ref.shape[0], factor_ref.shape[2] // BS
    rows_of, cols_of = nblock // per_row, nblock // per_col
    for r in range(per_row):
        for c in range(per_col):
            rb = r * rows_of + lax.axis_index("gx")
            cb = c * cols_of + lax.axis_index("gy")
            k = spot(cb // 2, jnp.maximum(rb // 2, cb // 2))
            rows = pl.ds(pl.multiple_of((rb % 2) * BS, BS), BS)
            wide = wh[k, rows, :].astype(jnp.float32) + wl[k, rows, :].astype(jnp.float32)
            block = jnp.where(cb % 2 == 0, wide[:, :BS], wide[:, BS:])
            inside = row + rb * BS >= col + cb * BS
            factor_ref[r, :, c * BS : (c + 1) * BS] = jnp.where(inside, block, 0.0)


def make_design(nblock, blocks_ref, coef_ref, design):
    slots = coef_ref.shape[0]
    rows = coef_ref.shape[1]
    chunk = 128

    @pl.loop(0, rows // chunk)
    def _(t):
        at = pl.ds(pl.multiple_of(t * chunk, chunk), chunk)
        idx = blocks_ref[at, :]
        labels = [jnp.broadcast_to(idx[:, s : s + 1], (chunk, BS)) for s in range(slots)]
        values = [coef_ref[s, at, :].astype(jnp.float32) for s in range(slots)]
        for b in range(nblock):
            total = jnp.where(labels[0] == b, values[0], 0.0)
            for s in range(1, slots):
                total = jnp.where(labels[s] == b, values[s], total)
            design[at, b * BS : (b + 1) * BS] = total.astype(jnp.bfloat16)


def make_rhs(nblock, scale, base, res_ref, design, term):
    rows = res_ref.shape[1]
    res = res_ref[...]
    high = res.astype(jnp.bfloat16)
    rest = res - high.astype(jnp.float32)
    mid = rest.astype(jnp.bfloat16)
    low = (rest - mid.astype(jnp.float32)).astype(jnp.bfloat16)
    row = lax.broadcasted_iota(jnp.int32, (16, rows), 0)
    parts = jnp.where(
        row == 0,
        high.astype(jnp.float32),
        jnp.where(
            row == 1,
            mid.astype(jnp.float32),
            jnp.where(row == 2, low.astype(jnp.float32), 0.0),
        ),
    ).astype(jnp.bfloat16)
    for b in range(nblock // 2):
        part = mm(parts, design[:, b * SB : (b + 1) * SB], 1, 0, None)
        total = jnp.sum(part, axis=0, keepdims=True) * scale
        term[base + 2 * b : base + 2 * b + 1, :] = total[:, :BS]
        term[base + 2 * b + 1 : base + 2 * b + 2, :] = total[:, BS:]


def gram_panel(nblock, scale, jj, begin, design, term):
    nsuper = nblock // 2
    right = design[:, jj * SB : (jj + 1) * SB]
    second = begin + BS * (nblock - 2 * jj)
    block = mm(right, right, 0, 0, None) * scale
    term[begin : begin + SB, :] = block[:, :BS]
    term[second : second + BS, :] = block[BS:, BS:]

    @pl.loop(jj + 1, nsuper)
    def _(ii):
        left = design[:, pl.ds(pl.multiple_of(ii * SB, SB), SB)]
        block = mm(left, design[:, jj * SB : (jj + 1) * SB], 0, 0, None) * scale
        down = (ii - jj) * SB
        term[pl.ds(pl.multiple_of(begin + down, BS), SB), :] = block[:, :BS]
        term[pl.ds(pl.multiple_of(second + down - BS, BS), SB), :] = block[:, BS:]


def exchanger(chunks, term_ref, out_ref, acc, recv, sends, recvs):
    gx, gy, gz = lax.axis_index("gx"), lax.axis_index("gy"), lax.axis_index("gz")
    x, ylo = gx % 4, gx // 4
    z, core = gy // 2, gy % 2

    def flip(v):
        return v + 1 - 2 * (v % 2)

    def gray(v):
        return (v % 2) + (v // 2) - 2 * (v % 2) * (v // 2)

    y = 2 * gz + ylo
    ynext = 4 * (1 - ylo)
    partner = [
        {"gx": 4 * ylo + flip(x)},
        {"gx": ynext + x},
        {"gy": 2 * flip(z) + core},
        {"gx": 4 * ylo + 3 - x},
        {"gx": ynext + x, "gz": 1 - gz},
        {"gy": 2 * (3 - z) + core},
    ]
    bit = [gray(x), gray(y), gray(z), x // 2, y // 2, z // 2]
    mate = {"gy": 2 * z + 1 - core}
    rows = lambda at, size: pl.ds(pl.multiple_of(at, SUB), size)

    def remote(src, dst, c, s, p, device):
        return pltpu.make_async_remote_copy(
            src_ref=src,
            dst_ref=dst,
            send_sem=sends.at[c, s, p],
            recv_sem=recvs.at[c, s, p],
            device_id=device,
            device_id_type=pl.DeviceIdType.MESH,
        )

    def chunk(c):
        base, size, _ = chunks[c]
        half, part = size // 2, size // 12
        pending = {}
        where = [0] * 6

        def stage(s):
            for p in range(6):
                local = base // 2 + p * part
                whole = base + core * half + p * part
                span = part >> min(s, HALVE)
                if s == 0:
                    other = base + (1 - core) * half + p * part
                    copy = remote(
                        term_ref.at[rows(other, part), :],
                        acc.at[local : local + part, :],
                        c, 0, p, mate,
                    )
                    copy.start()
                    pending[0, p] = copy
                    continue
                pending[s - 1, p].wait_recv()
                if s == 1:
                    acc[local : local + part, :] = (
                        term_ref[rows(whole, part), :] + acc[local : local + part, :]
                    )
                    span = part
                elif s <= 2 * HALVE + 1:
                    got = part >> min(s - 1, HALVE)
                    at = rows(local + where[p], got)
                    slot = slots[s - 1] + base // 12 // (part // got) * 6 + p * got
                    if s - 1 > HALVE:
                        pending[s - 1, p].wait_send()
                    total = acc[at, :] + recv[slot : slot + got, :]
                    if s <= 2 * HALVE:
                        acc[at, :] = total
                    else:
                        out_ref[rows(whole + where[p], got), :] = total
                    span = got
                if s <= HALVE:
                    g = (p + s - 1) % 6
                    span = part >> s
                    keep = where[p] + bit[g] * span
                    give = where[p] + (1 - bit[g]) * span
                    slot = slots[s] + base // 12 // (part // span) * 6 + p * span
                    copy = remote(
                        acc.at[rows(local + give, span), :],
                        recv.at[slot : slot + span, :],
                        c, s, p, partner[g],
                    )
                    where[p] = keep
                elif s <= 2 * HALVE:
                    g = (p + s - 1) % 6
                    slot = slots[s] + base // 12 // (part // span) * 6 + p * span
                    copy = remote(
                        acc.at[rows(local + where[p], span), :],
                        recv.at[slot : slot + span, :],
                        c, s, p, partner[g],
                    )
                elif s <= 3 * HALVE:
                    level = 3 * HALVE + 1 - s
                    g = (p + level - 1) % 6
                    span = part >> level
                    block = out_ref.at[rows(whole + where[p], span), :]
                    copy = remote(block, block, c, s, p, partner[g])
                    where[p] = where[p] - bit[g] * span
                elif s == 3 * HALVE + 1:
                    block = out_ref.at[rows(whole, part), :]
                    copy = remote(block, block, c, s, p, mate)
                else:
                    continue
                copy.start()
                pending[s, p] = copy

        def finish():
            for (s, p), copy in pending.items():
                if not HALVE < s <= 2 * HALVE:
                    copy.wait_send()

        return stage, finish

    slots, at = {}, 0
    total = sum(size for _, size, _ in chunks) // 2
    for s in range(1, 2 * HALVE + 1):
        slots[s] = at
        at += total >> min(s, HALVE)
    runs = [chunk(c) for c in range(len(chunks))]

    def turn(t, delays):
        for (stage, _), delay in zip(runs, delays):
            if 0 <= t - delay <= 3 * HALVE + 2:
                stage(t - delay)

    def finish():
        for _, close in runs:
            close()

    def greet():
        barrier = pltpu.get_barrier_semaphore()
        for device in partner + [mate]:
            pl.semaphore_signal(
                barrier, inc=1, device_id=device, device_id_type=pl.DeviceIdType.MESH
            )

    def meet():
        pl.semaphore_wait(pltpu.get_barrier_semaphore(), len(partner) + 1)

    return turn, finish, greet, meet


DELAYS = (0, 2, 4)


def whole_kernel(
    nblock, scale, blocks_ref, coef_ref, res_ref, factor_ref, z_ref,
    design, term, acc, recv, out, wh, wl, tiles, y, inv_h, inv_l, sends, recvs,
):
    nsuper = nblock // 2
    begins, rhs, chunks, _ = layout(nblock)
    turn, finish, greet, meet = exchanger(chunks, term, out, acc, recv, sends, recvs)
    greet()
    for base, size, used in chunks:
        if used < base + size:
            term[used : base + size, :] = jnp.zeros((base + size - used, BS), jnp.float32)

    def gram(j):
        gram_panel(nblock, scale, j, begins[j], design, term)

    make_design(nblock, blocks_ref, coef_ref, design)
    make_rhs(nblock, scale, rhs, res_ref, design, term)
    gram(0)
    gram(nsuper - 1)
    meet()
    work = {0: (1,), 1: (2,), 2: (3,), 3: range(4, nsuper - 1)}
    ready = 3 * HALVE + 2
    for t in range(ready + 1):
        turn(t, DELAYS)
        for j in work.get(t, ()):
            gram(j)

    def pivot_hook(n):
        if n == 5:
            turn(ready + 1, DELAYS)
        if n == 11:
            turn(ready + 2, DELAYS)

    def second_hook():
        turn(ready + 4, DELAYS)
        finish()

    hooks = {"pivot": pivot_hook, "solved": lambda: turn(ready + 3, DELAYS), "second": second_hook}
    factor_all(nblock, begins, rhs, out, factor_ref, z_ref, wh, wl, tiles, y, inv_h, inv_l, hooks)


def on_device(blocks, coefficients, residuals):
    row_count = lax.axis_size("gx")
    col_count = lax.axis_size("gy")
    devices = row_count * col_count * lax.axis_size("gz")
    rows, slots, width = coefficients.shape
    scale = 1.0 / (rows * devices)
    nblock = G // width
    nsuper = nblock // 2
    _, _, chunks, total = layout(nblock)
    half = total // 2
    landing = sum(half >> min(s, HALVE) for s in range(1, 2 * HALVE + 1))
    per_row, per_col = nblock // row_count, nblock // col_count
    vmem = pl.BlockSpec(memory_space=pltpu.VMEM)
    sem = pltpu.SemaphoreType.DMA((len(chunks), 3 * HALVE + 2, 6))
    count = nsuper * (nsuper + 1) // 2
    factor, answer = pl.pallas_call(
        functools.partial(whole_kernel, nblock, scale),
        out_shape=(
            jax.ShapeDtypeStruct((per_row, width, per_col * width), jnp.float32),
            jax.ShapeDtypeStruct((nblock, width), jnp.float32),
        ),
        in_specs=[vmem] * 3,
        out_specs=(vmem, vmem),
        scratch_shapes=[
            pltpu.VMEM((rows, G), jnp.bfloat16),
            pltpu.VMEM((total, width), jnp.float32),
            pltpu.VMEM((half, width), jnp.float32),
            pltpu.VMEM((landing, width), jnp.float32),
            pltpu.VMEM((total, width), jnp.float32),
            pltpu.VMEM((count, SB, SB), jnp.bfloat16),
            pltpu.VMEM((count, SB, SB), jnp.bfloat16),
            pltpu.VMEM((2, G + SB, SB), jnp.float32),
            pltpu.VMEM((nsuper, SUB, SB), jnp.float32),
            pltpu.VMEM((nsuper, SB, SB), jnp.bfloat16),
            pltpu.VMEM((nsuper, SB, SB), jnp.bfloat16),
            sem,
            sem,
        ],
        compiler_params=pltpu.CompilerParams(
            vmem_limit_bytes=VMEM_LIMIT, has_side_effects=True, collective_id=0
        ),
    )(blocks, coefficients.transpose(1, 0, 2), residuals.reshape(1, rows))
    return (factor.reshape(1, per_row, width, 1, per_col, width), answer)


def solution(mesh):
    in_specs = (
        P(("gx", "gy", "gz"), None),
        P(("gx", "gy", "gz"), None, None),
        P(("gx", "gy", "gz")),
    )
    out_specs = (P("gx", None, None, "gy", None, None), P())
    return jax.shard_map(
        on_device, mesh=mesh, in_specs=in_specs, out_specs=out_specs, check_vma=False
    )
```

```python
import functools

import jax
import jax.numpy as jnp
from jax import lax
from jax.experimental import pallas as pl
from jax.experimental.pallas import tpu as pltpu
from jax.sharding import PartitionSpec as P

G = 2048
BS = 128
SB = 2 * BS
SUB = 8
HB = BS // 2
VMEM_LIMIT = 63 * 1024 * 1024
UNIT = 2 * 6 * 8 * SUB
HALVE = 3
PIECES = ((2, 4), (9,), (9,))


def mm(a, b, ca, cb, precision=lax.Precision.HIGHEST):
    return lax.dot_general(
        a, b, (((ca,), (cb,)), ((), ())), precision=precision, preferred_element_type=jnp.float32
    )

def split(x):
    high = x.astype(jnp.bfloat16)
    return high, (x - high.astype(jnp.float32)).astype(jnp.bfloat16)

def mm3(a, b, ca, cb):
    ah, al = a if isinstance(a, tuple) else split(a)
    bh, bl = b if isinstance(b, tuple) else split(b)
    return mm(
        jnp.concatenate([ah, ah, al], axis=ca), jnp.concatenate([bh, bl, bh], axis=cb), ca, cb, None
    )

def panel_start(nblock, k):
    return BS * (nblock * k - (k * (k - 1)) // 2)

def chol_half(x, off, fill):
    shape = (SUB, BS)
    sub = lax.broadcasted_iota(jnp.int32, shape, 0)
    count = len(x)
    x = list(x)

    def lane(v, j):
        return jnp.broadcast_to(v[:, off + j : off + j + 1], shape)

    def sublane(v, j):
        return jnp.broadcast_to(v[j : j + 1, :], shape)

    def lanes(v, p):
        return [lane(v, p * SUB + j) for j in range(SUB)]

    cols = lanes(x[0], 0)
    ahead = lanes(x[1], 1)
    below = {i: lanes(x[i], 0) for i in range(1, count)}
    for p in range(count):
        if p % 2 == 1:
            fill()
        block = x[p]
        scales, rows, upper = [], [], {}
        for j in range(SUB):
            inv = lax.rsqrt(sublane(cols[j], j))
            mult = jnp.where(sub > j, cols[j] * inv, 0.0)
            for k in range(j + 1, SUB):
                upper[j, k] = sublane(cols[k], j) * inv
                cols[k] = cols[k] - mult * upper[j, k]
            row = sublane(block, j) * inv
            block = jnp.where(sub == j, row, block - mult * row)
            scales.append(inv)
            rows.append(row)
        x[p] = block
        fresh, reach = {}, None
        for i in range(p + 1, count):
            b = below[i]
            mults = []
            for j in range(SUB):
                m = b[j] * scales[j]
                mults.append(m)
                for k in range(j + 1, SUB):
                    b[k] = b[k] - m * upper[j, k]
            if i == p + 1:
                for k in range(SUB):
                    for j in range(SUB):
                        ahead[k] = ahead[k] - mults[j] * sublane(mults[j], k)
            for j in range(SUB):
                x[i] = x[i] - mults[j] * rows[j]
            if i > p + 1:
                fresh[i] = lanes(x[i], p + 1)
                if i == p + 2:
                    reach = lanes(x[i], p + 2)
        cols, ahead, below = ahead, reach, fresh
    return x

def chol_block(t, fill=lambda: None):
    row = lax.broadcasted_iota(jnp.int32, (BS, BS), 0)
    col = lax.broadcasted_iota(jnp.int32, (BS, BS), 1)
    hrow, hcol = row[:HB], col[:HB]

    def rowsof(v):
        return [v[i * SUB : (i + 1) * SUB, :] for i in range(HB // SUB)]

    zero = jnp.zeros((HB, BS), jnp.float32)
    top = t[:HB]
    first = jnp.where(hcol < HB, top, jnp.where(hcol - HB == hrow, 1.0, 0.0))
    xa = jnp.concatenate(chol_half(rowsof(first), 0, fill), axis=0)
    ea = jnp.where((hcol >= HB) & (hcol - HB <= hrow), xa, 0.0)
    ua = mm3(ea, jnp.concatenate([zero, top], axis=0), 1, 0)
    u12 = split(jnp.where(hcol >= HB, ua, 0.0))
    low = t[HB:] - mm3(u12, u12, 0, 0)[HB:]
    second = jnp.where(hcol >= HB, low, jnp.where(hcol == hrow, 1.0, 0.0))
    xb = jnp.concatenate(chol_half(rowsof(second), HB, fill), axis=0)
    eb = jnp.where(hcol <= hrow, xb, 0.0)
    w = mm3(u12, ea, 0, 0)[HB:]
    e21 = mm3(eb, jnp.concatenate([w, zero], axis=0), 1, 0)
    lowrow = jnp.where(hcol < HB, eb, -e21)
    inverse = pltpu.roll(jnp.concatenate([ea, lowrow], axis=0), HB, 1)
    upper = jnp.concatenate([jnp.where(hcol < HB, jnp.where(hrow <= hcol, xa, 0.0), ua),
                             jnp.where(hcol - HB >= hrow, xb, 0.0)], axis=0)
    return upper.T, inverse

def layout(nblock):
    nsuper = nblock // 2
    sizes = [BS * (2 * nblock - 4 * j - 1) for j in range(nsuper)]
    begins, chunks, pads, at = {}, [], [], 0
    for group, pieces in zip(((0, nsuper - 1), (1, 2), range(3, nsuper - 1)), PIECES):
        base = at
        for j in group:
            begins[j] = at
            at += sizes[j]
        if base == 0:
            rhs = at
            at += nblock
        pads.append((at, base + UNIT * sum(pieces)))
        at = base
        for piece in pieces:
            chunks.append((at, UNIT * piece))
            at += UNIT * piece
    return begins, rhs, chunks, pads, at


def sides(nblock, begins, j):
    left = begins[j] - j * SB
    return left, left + BS * (nblock - 2 * j - 1)


def factor_all(nblock, begins, rhs, packed, factor_ref, z_ref, wh, wl, tiles, y, inv_h, inv_l, hook):
    nsuper = nblock // 2
    spare = nsuper * (nsuper + 1) // 2

    def at(ii):
        return pl.ds(pl.multiple_of(ii * SB, SB), SB)

    def spot(j, ii):
        return (j * (2 * nsuper + 1 - j)) // 2 + ii - j

    def both(j, ii):
        k = spot(j, ii)
        return wh[k], wl[k]

    def fetch(kk):
        if isinstance(kk, int):
            first, second = sides(nblock, begins, kk)
        else:
            first, second = (jnp.int32(v) for v in sides(nblock, begins, 1))
            for j in range(2, nsuper):
                left, right = sides(nblock, begins, j)
                first = jnp.where(kk == j, left, first)
                second = jnp.where(kk == j, right, second)

        @pl.loop(kk, nsuper)
        def _(ii):
            for side, begin in enumerate((first, second)):
                rows = pl.ds(pl.multiple_of(begin + ii * SB, BS), SB)
                tiles[kk % 3, at(ii), side * BS : (side + 1) * BS] = packed[rows, :]

    def fetch_first(low, high):
        @pl.loop(low, high)
        def _(ii):
            for side in range(2):
                rows = pl.ds(pl.multiple_of(2 * SB * ii - BS + side * SB, BS), SB)
                tiles[0, at(ii), side * BS : (side + 1) * BS] = packed[rows, :]

    row = lax.broadcasted_iota(jnp.int32, (BS, BS), 0)
    col = lax.broadcasted_iota(jnp.int32, (BS, BS), 1)
    zero = jnp.zeros((BS, BS), jnp.float32)
    for side in range(3):
        tiles[side, nsuper * SB :, :] = jnp.zeros((SB, SB), jnp.float32)
    y[nsuper] = jnp.zeros((SUB, SB), jnp.float32)
    tiles[0, 0:SB, 0:BS] = packed[0:SB, :]
    tiles[0, 0:SB, BS:SB] = packed[BS : BS + SB, :]
    fetch_first(1, 2)

    def pivot(kk, here, fill):
        diag = tiles[here, at(kk), :]
        la, ea = chol_block(diag[0:BS, 0:BS], fill)
        eas = split(ea)
        l21 = mm3(diag[BS:SB, 0:BS], eas, 1, 1)
        l21s = split(l21)
        lb, eb = chol_block(diag[BS:SB, BS:SB] - mm3(l21s, l21s, 1, 1), fill)
        ec = -mm3(eb, mm3(l21s, eas, 1, 0), 1, 0)
        inv = split(jnp.concatenate(
            [jnp.concatenate([ea, zero], axis=1), jnp.concatenate([ec, eb], axis=1)], axis=0))
        low = jnp.concatenate(
            [jnp.concatenate([la, zero], axis=1), jnp.concatenate([l21, lb], axis=1)], axis=0)
        k = spot(kk, kk)
        wh[k], wl[k] = split(low)
        inv_h[kk], inv_l[kk] = inv
        return inv

    early = iter(range(2 * SUB))
    inv = pivot(0, 0, lambda: hook("pivot%d" % next(early)))
    side = split(mm3(tiles[0, at(1), :], inv, 1, 1))
    wh[1], wl[1] = side
    hook("solved")
    fetch_first(2, nsuper)
    for b in range(nblock):
        y[b // 2, 0:1, (b % 2) * BS : (b % 2 + 1) * BS] = packed[rhs + b : rhs + b + 1, :]
        if b % 2 == 0:
            y[b // 2, 1:SUB, :] = jnp.zeros((SUB - 1, SB), jnp.float32)
    y[0] = mm3(y[0], (inv_h[0], inv_l[0]), 1, 1)
    fetch(1)
    side = both(0, 1)
    tiles[1, at(1), :] = tiles[1, at(1), :] - mm3(side, side, 1, 1)
    fetch(2)

    @pl.loop(1, nsuper)
    def _(kk):
        last = kk - 1
        prev, here, there = (kk + 2) % 3, kk % 3, (kk + 1) % 3
        rest = nsuper - 1 - kk
        final = nsuper - 1
        cursor = [kk + 1, 0]

        def follow(n):
            ii = kk + 1 + n
            valid = ii < nsuper
            value = split(
                mm3(tiles[prev, at(jnp.minimum(ii, final)), :], (inv_h[last], inv_l[last]), 1, 1)
            )
            k = jnp.where(valid, spot(last, ii), spare)
            wh[k], wl[k] = value
            k = jnp.where(valid, ii, nsuper)
            y[k] = y[k] - mm3(y[last], value, 1, 1)

        def update(n):
            first = n < rest
            ii2, j2 = cursor
            valid = first | (ii2 < nsuper)
            j = jnp.where(valid, jnp.where(first, last, j2), 0)
            ii = jnp.where(valid, jnp.where(first, kk + 1 + n, ii2), 0)
            other = jnp.where(valid, jnp.where(first, kk, kk + 1), 0)
            side = jnp.where(valid, jnp.where(first, here, there), 0)
            dest = jnp.where(valid, ii, nsuper)
            moved = jnp.where(first, j2, j2 + 1)
            done = jnp.logical_not(first) & (moved >= kk)
            cursor[0] = jnp.where(done, ii2 + 1, ii2)
            cursor[1] = jnp.where(done, 0, moved)
            tiles[side, at(dest), :] = tiles[side, at(dest), :] - mm3(both(j, ii), both(j, other), 1, 1)

        plan = [[functools.partial(follow, 2 * n), functools.partial(follow, 2 * n + 1)] for n in range(3)]
        plan += [[functools.partial(update, 2 * n), functools.partial(update, 2 * n + 1)] for n in range(3)]
        plan += [[functools.partial(update, n)] for n in range(6, 2 * SUB)]
        steps = iter(plan)

        def fill():
            for f in next(steps):
                f()

        for step in (1, 2):

            @pl.when(kk == step)
            def _():
                hook("first%d" % step)

        ykk = y[kk] - mm3(y[last], both(last, kk), 1, 1)
        inv = pivot(kk, here, fill)
        y[kk] = mm3(ykk, inv, 1, 1)
        value = split(mm3(tiles[here, at(jnp.minimum(kk + 1, final)), :], inv, 1, 1))
        k = jnp.where(kk < final, spot(kk, kk + 1), spare)
        wh[k], wl[k] = value
        dest = jnp.where(kk < final, kk + 1, nsuper)
        tiles[there, at(dest), :] = tiles[there, at(dest), :] - mm3(value, value, 1, 1)

        for step in (1, 2):

            @pl.when(kk == step)
            def _():
                hook("last%d" % step)

        @pl.when(kk + 2 < nsuper)
        def _():
            fetch(kk + 2)

    state = [y[j] for j in range(nsuper)]
    for kk in reversed(range(nsuper)):
        state[kk] = mm3(state[kk], (inv_h[kk], inv_l[kk]), 1, 0)
        x = split(state[kk])
        for j in reversed(range(kk)):
            state[j] = state[j] - mm3(x, both(j, kk), 1, 0)
    for b in range(nblock):
        z_ref[b : b + 1, :] = state[b // 2][0:1, (b % 2) * BS : (b % 2 + 1) * BS]

    per_row, per_col = factor_ref.shape[0], factor_ref.shape[2] // BS
    rows_of, cols_of = nblock // per_row, nblock // per_col
    for r in range(per_row):
        for c in range(per_col):
            rb = r * rows_of + lax.axis_index("gx")
            cb = c * cols_of + lax.axis_index("gy")
            k = spot(cb // 2, jnp.maximum(rb // 2, cb // 2))
            rows = pl.ds(pl.multiple_of((rb % 2) * BS, BS), BS)
            wide = wh[k, rows, :].astype(jnp.float32) + wl[k, rows, :].astype(jnp.float32)
            block = jnp.where(cb % 2 == 0, wide[:, :BS], wide[:, BS:])
            inside = row + rb * BS >= col + cb * BS
            factor_ref[r, :, c * BS : (c + 1) * BS] = jnp.where(inside, block, 0.0)


def make_design(nblock, blocks_ref, coef_ref, design, wide):
    slots, rows = blocks_ref.shape
    chunk = 128

    @pl.loop(0, rows // chunk)
    def _(t):
        at = pl.ds(pl.multiple_of(t * chunk, chunk), chunk)
        idx = blocks_ref[:, at]
        idx = jnp.concatenate([idx] * (SUB // slots), axis=0).T
        labels = [jnp.broadcast_to(idx[:, s : s + 1], (chunk, BS)) for s in range(slots)]
        span = chunk * slots
        wide[...] = coef_ref[pl.ds(pl.multiple_of(t * span, span), span), :].astype(jnp.float32)
        values = [wide[pl.ds(s, chunk, stride=slots), :] for s in range(slots)]
        for b in range(nblock):
            total = jnp.where(labels[0] == b, values[0], 0.0)
            for s in range(1, slots):
                total = jnp.where(labels[s] == b, values[s], total)
            design[at, b * BS : (b + 1) * BS] = total.astype(jnp.bfloat16)


def make_rhs(nblock, scale, base, res_ref, design, term):
    rows = res_ref.shape[1]
    res = res_ref[...]
    high = res.astype(jnp.bfloat16)
    rest = res - high.astype(jnp.float32)
    mid = rest.astype(jnp.bfloat16)
    low = (rest - mid.astype(jnp.float32)).astype(jnp.bfloat16)
    row = lax.broadcasted_iota(jnp.int32, (16, rows), 0)
    parts = jnp.where(
        row == 0,
        high.astype(jnp.float32),
        jnp.where(
            row == 1,
            mid.astype(jnp.float32),
            jnp.where(row == 2, low.astype(jnp.float32), 0.0),
        ),
    ).astype(jnp.bfloat16)
    for b in range(nblock // 2):
        part = mm(parts, design[:, b * SB : (b + 1) * SB], 1, 0, None)
        total = jnp.sum(part, axis=0, keepdims=True) * scale
        term[base + 2 * b : base + 2 * b + 1, :] = total[:, :BS]
        term[base + 2 * b + 1 : base + 2 * b + 2, :] = total[:, BS:]


def gram_panel(nblock, scale, jj, begins, design, term, low, high):
    first, second = sides(nblock, begins, jj)
    right = design[:, jj * SB : (jj + 1) * SB]
    if low == jj:
        begin = begins[jj]
        block = mm(right, right, 0, 0, None) * scale
        term[begin : begin + SB, :] = block[:, :BS]
        begin = SB if jj == 0 else second + jj * SB + BS
        term[begin : begin + BS, :] = block[BS:, BS:]

    @pl.loop(max(low, jj + 1), high)
    def _(ii):
        left = design[:, pl.ds(pl.multiple_of(ii * SB, SB), SB)]
        block = mm(left, design[:, jj * SB : (jj + 1) * SB], 0, 0, None) * scale
        near = 2 * SB * ii - BS if jj == 0 else first + ii * SB
        far = 2 * SB * ii + BS if jj == 0 else second + ii * SB
        term[pl.ds(pl.multiple_of(near, BS), SB), :] = block[:, :BS]
        term[pl.ds(pl.multiple_of(far, BS), SB), :] = block[:, BS:]


def exchanger(chunks, term_ref, out_ref, acc, recv, sends, recvs):
    gx, gy, gz = lax.axis_index("gx"), lax.axis_index("gy"), lax.axis_index("gz")
    x, ylo = gx % 4, gx // 4
    z, core = gy // 2, gy % 2

    def flip(v):
        return v + 1 - 2 * (v % 2)

    def gray(v):
        return (v % 2) + (v // 2) - 2 * (v % 2) * (v // 2)

    y = 2 * gz + ylo
    ynext = 4 * (1 - ylo)
    partner = [
        {"gx": 4 * ylo + flip(x)},
        {"gx": ynext + x},
        {"gy": 2 * flip(z) + core},
        {"gx": 4 * ylo + 3 - x},
        {"gx": ynext + x, "gz": 1 - gz},
        {"gy": 2 * (3 - z) + core},
    ]
    bit = [gray(x), gray(y), gray(z), x // 2, y // 2, z // 2]
    mate = {"gy": 2 * z + 1 - core}
    rows = lambda at, size: pl.ds(pl.multiple_of(at, SUB), size)

    def remote(src, dst, c, s, p, device):
        return pltpu.make_async_remote_copy(
            src_ref=src,
            dst_ref=dst,
            send_sem=sends.at[c, s, p],
            recv_sem=recvs.at[c, s, p],
            device_id=device,
            device_id_type=pl.DeviceIdType.MESH,
        )

    slots, at = {}, 0
    total = sum(size for _, size in chunks) // 2
    for s in range(1, 2 * HALVE + 1):
        slots[s] = at
        at += total >> min(s, HALVE)

    def chunk(c):
        base, size = chunks[c]
        half, part = size // 2, size // 12
        local = [base // 2 + p * part for p in range(6)]
        whole = [base + core * half + p * part for p in range(6)]
        other = [base + (1 - core) * half + p * part for p in range(6)]
        where = []
        for p in range(6):
            steps = [0]
            for level in range(1, HALVE + 1):
                steps.append(steps[-1] + bit[(p + level - 1) % 6] * (part >> level))
            where.append(steps)

        def landing(s, p):
            span = part >> min(s, HALVE)
            slot = slots[s] + ((base // 2) >> min(s, HALVE)) + p * span
            return slice(slot, slot + span)

        def copy(s, p):
            if s == 0:
                src = term_ref.at[rows(other[p], part), :]
                dst = acc.at[local[p] : local[p] + part, :]
                return remote(src, dst, c, 0, p, mate)
            if s <= HALVE:
                span, g = part >> s, (p + s - 1) % 6
                give = where[p][s - 1] + (1 - bit[g]) * span
                src = acc.at[rows(local[p] + give, span), :]
                return remote(src, recv.at[landing(s, p), :], c, s, p, partner[g])
            if s <= 2 * HALVE:
                span, g = part >> HALVE, (p + s - 1) % 6
                src = acc.at[rows(local[p] + where[p][HALVE], span), :]
                return remote(src, recv.at[landing(s, p), :], c, s, p, partner[g])
            level = 3 * HALVE + 1 - s
            block = out_ref.at[rows(whole[p] + where[p][level], part >> level), :]
            device = partner[(p + level - 1) % 6] if level else mate
            return remote(block, block, c, s, p, device)

        def stage(s):
            for p in range(6):
                if s:
                    copy(s - 1, p).wait_recv()
                if s == 1:
                    at = slice(local[p], local[p] + part)
                    acc[at, :] = term_ref[rows(whole[p], part), :] + acc[at, :]
                elif 1 < s <= 2 * HALVE + 1:
                    level = min(s - 1, HALVE)
                    span = part >> level
                    at = rows(local[p] + where[p][level], span)
                    if s - 1 > HALVE:
                        copy(s - 1, p).wait_send()
                    total = acc[at, :] + recv[landing(s - 1, p), :]
                    if s <= 2 * HALVE:
                        acc[at, :] = total
                    else:
                        out_ref[rows(whole[p] + where[p][level], span), :] = total
                if s <= 3 * HALVE + 1:
                    copy(s, p).start()

        def finish():
            for s in range(3 * HALVE + 2):
                if not HALVE < s <= 2 * HALVE:
                    for p in range(6):
                        copy(s, p).wait_send()

        return stage, finish

    runs = [chunk(c) for c in range(len(chunks))]

    def turn(t):
        for (stage, _), rounds in zip(runs, ROUNDS):
            for s, at in enumerate(rounds):
                if at == t:
                    stage(s)

    def finish():
        for _, close in runs:
            close()

    def greet():
        barrier = pltpu.get_barrier_semaphore()
        for device in partner + [mate]:
            pl.semaphore_signal(
                barrier, inc=1, device_id=device, device_id_type=pl.DeviceIdType.MESH
            )

    def meet():
        pl.semaphore_wait(pltpu.get_barrier_semaphore(), len(partner) + 1)

    return turn, finish, greet, meet


ROUNDS = (
    (0, 1, 2, 3, 4, 5, 6, 7, 8, 9, 10, 11),
    (1, 2, 3, 4, 5, 6, 7, 8, 9, 10, 11, 12),
    (2, 3, 4, 5, 6, 7, 8, 9, 10, 11, 12, 13),
    (5, 6, 7, 8, 9, 10, 11, 12, 13, 14, 15, 16),
)
READY = 11
WORK = {0: (0,), 1: (1, 2), 2: (3,), 3: (4,), 4: (5, 6)}
TURNS = {'pivot8': (12,), 'solved': (13,), 'first1': (14,), 'last1': (15, 16)}


def whole_kernel(
    nblock, scale, blocks_ref, coef_ref, res_ref, factor_ref, z_ref,
    design, wide, term, acc, recv, out, wh, wl, tiles, y, inv_h, inv_l, sends, recvs,
):
    nsuper = nblock // 2
    begins, rhs, chunks, pads, _ = layout(nblock)
    turn, finish, greet, meet = exchanger(chunks, term, out, acc, recv, sends, recvs)
    greet()
    for used, end in pads:
        if used < end:
            term[used:end, :] = jnp.zeros((end - used, BS), jnp.float32)

    def gram(j, low=None, high=nsuper):
        gram_panel(nblock, scale, j, begins, design, term, j if low is None else low, high)

    make_design(nblock, blocks_ref, coef_ref, design, wide)
    gram(0, 0, 4)
    meet()
    for t in range(READY + 1):
        turn(t)
        for j in WORK.get(t, ()):
            if j == 0:
                gram(0, 4)
                gram(nsuper - 1)
                make_rhs(nblock, scale, rhs, res_ref, design, term)
            else:
                gram(j)

    def hook(name):
        for t in TURNS.get(name, ()):
            turn(t)

    factor_all(nblock, begins, rhs, out, factor_ref, z_ref, wh, wl, tiles, y, inv_h, inv_l, hook)
    finish()


def on_device(blocks, coefficients, residuals):
    row_count = lax.axis_size("gx")
    col_count = lax.axis_size("gy")
    devices = row_count * col_count * lax.axis_size("gz")
    rows, slots, width = coefficients.shape
    scale = 1.0 / (rows * devices)
    nblock = G // width
    nsuper = nblock // 2
    _, _, chunks, _, total = layout(nblock)
    half = total // 2
    landing = sum(half >> min(s, HALVE) for s in range(1, 2 * HALVE + 1))
    per_row, per_col = nblock // row_count, nblock // col_count
    vmem = pl.BlockSpec(memory_space=pltpu.VMEM)
    sem = pltpu.SemaphoreType.DMA((len(chunks), 3 * HALVE + 2, 6))
    count = nsuper * (nsuper + 1) // 2
    factor, answer = pl.pallas_call(
        functools.partial(whole_kernel, nblock, scale),
        out_shape=(
            jax.ShapeDtypeStruct((per_row, width, per_col * width), jnp.float32),
            jax.ShapeDtypeStruct((nblock, width), jnp.float32),
        ),
        in_specs=[vmem] * 3,
        out_specs=(vmem, vmem),
        scratch_shapes=[
            pltpu.VMEM((rows, G), jnp.bfloat16),
            pltpu.VMEM((BS * slots, width), jnp.float32),
            pltpu.VMEM((total, width), jnp.float32),
            pltpu.VMEM((half, width), jnp.float32),
            pltpu.VMEM((landing, width), jnp.float32),
            pltpu.VMEM((total, width), jnp.float32),
            pltpu.VMEM((count + 1, SB, SB), jnp.bfloat16),
            pltpu.VMEM((count + 1, SB, SB), jnp.bfloat16),
            pltpu.VMEM((3, G + SB, SB), jnp.float32),
            pltpu.VMEM((nsuper + 1, SUB, SB), jnp.float32),
            pltpu.VMEM((nsuper, SB, SB), jnp.bfloat16),
            pltpu.VMEM((nsuper, SB, SB), jnp.bfloat16),
            sem,
            sem,
        ],
        compiler_params=pltpu.CompilerParams(
            vmem_limit_bytes=VMEM_LIMIT, has_side_effects=True, collective_id=0
        ),
    )(blocks.T, coefficients.reshape(rows * slots, width), residuals.reshape(1, rows))
    return (factor.reshape(1, per_row, width, 1, per_col, width), answer)


def solution(mesh):
    in_specs = (
        P(("gx", "gy", "gz"), None),
        P(("gx", "gy", "gz"), None, None),
        P(("gx", "gy", "gz")),
    )
    out_specs = (P("gx", None, None, "gy", None, None), P())
    return jax.shard_map(
        on_device, mesh=mesh, in_specs=in_specs, out_specs=out_specs, check_vma=False
    )
```

```python
import functools

import jax
import jax.numpy as jnp
from jax import lax
from jax.experimental import pallas as pl
from jax.experimental.pallas import tpu as pltpu
from jax.sharding import PartitionSpec as P

G = 2048
BS = 128
SB = 2 * BS
SUB = 8
HB = BS // 2
VMEM_LIMIT = 63 * 1024 * 1024
UNIT = 2 * 6 * 8 * SUB
HALVE = 3
PIECES = ((2, 4), (9,), (9,))


def mm(a, b, ca, cb, precision=lax.Precision.HIGHEST):
    return lax.dot_general(
        a, b, (((ca,), (cb,)), ((), ())), precision=precision, preferred_element_type=jnp.float32
    )

def split(x):
    high = x.astype(jnp.bfloat16)
    return high, (x - high.astype(jnp.float32)).astype(jnp.bfloat16)

def mm3(a, b, ca, cb):
    ah, al = a if isinstance(a, tuple) else split(a)
    bh, bl = b if isinstance(b, tuple) else split(b)
    return mm(
        jnp.concatenate([ah, ah, al], axis=ca), jnp.concatenate([bh, bl, bh], axis=cb), ca, cb, None
    )

def panel_start(nblock, k):
    return BS * (nblock * k - (k * (k - 1)) // 2)

def chol_half(x, off, fill):
    shape = (SUB, BS)
    sub = lax.broadcasted_iota(jnp.int32, shape, 0)
    count = len(x)
    x = list(x)

    def lane(v, j):
        return jnp.broadcast_to(v[:, off + j : off + j + 1], shape)

    def sublane(v, j):
        return jnp.broadcast_to(v[j : j + 1, :], shape)

    def lanes(v, p):
        return [lane(v, p * SUB + j) for j in range(SUB)]

    cols = lanes(x[0], 0)
    ahead = lanes(x[1], 1)
    below = {i: lanes(x[i], 0) for i in range(1, count)}
    for p in range(count):
        if p % 2 == 1:
            fill()
        block = x[p]
        scales, rows, upper = [], [], {}
        for j in range(SUB):
            inv = lax.rsqrt(sublane(cols[j], j))
            mult = jnp.where(sub > j, cols[j] * inv, 0.0)
            for k in range(j + 1, SUB):
                upper[j, k] = sublane(cols[k], j) * inv
                cols[k] = cols[k] - mult * upper[j, k]
            row = sublane(block, j) * inv
            block = jnp.where(sub == j, row, block - mult * row)
            scales.append(inv)
            rows.append(row)
        x[p] = block
        fresh, reach = {}, None
        for i in range(p + 1, count):
            b = below[i]
            mults = []
            for j in range(SUB):
                m = b[j] * scales[j]
                mults.append(m)
                for k in range(j + 1, SUB):
                    b[k] = b[k] - m * upper[j, k]
            if i == p + 1:
                for k in range(SUB):
                    for j in range(SUB):
                        ahead[k] = ahead[k] - mults[j] * sublane(mults[j], k)
            for j in range(SUB):
                x[i] = x[i] - mults[j] * rows[j]
            if i > p + 1:
                fresh[i] = lanes(x[i], p + 1)
                if i == p + 2:
                    reach = lanes(x[i], p + 2)
        cols, ahead, below = ahead, reach, fresh
    return x

def chol_block(t, fill=lambda: None):
    row = lax.broadcasted_iota(jnp.int32, (BS, BS), 0)
    col = lax.broadcasted_iota(jnp.int32, (BS, BS), 1)
    hrow, hcol = row[:HB], col[:HB]

    def rowsof(v):
        return [v[i * SUB : (i + 1) * SUB, :] for i in range(HB // SUB)]

    zero = jnp.zeros((HB, BS), jnp.float32)
    top = t[:HB]
    first = jnp.where(hcol < HB, top, jnp.where(hcol - HB == hrow, 1.0, 0.0))
    xa = jnp.concatenate(chol_half(rowsof(first), 0, fill), axis=0)
    ea = jnp.where((hcol >= HB) & (hcol - HB <= hrow), xa, 0.0)
    ua = mm3(ea, jnp.concatenate([zero, top], axis=0), 1, 0)
    u12 = split(jnp.where(hcol >= HB, ua, 0.0))
    low = t[HB:] - mm3(u12, u12, 0, 0)[HB:]
    second = jnp.where(hcol >= HB, low, jnp.where(hcol == hrow, 1.0, 0.0))
    xb = jnp.concatenate(chol_half(rowsof(second), HB, fill), axis=0)
    eb = jnp.where(hcol <= hrow, xb, 0.0)
    w = mm3(u12, ea, 0, 0)[HB:]
    e21 = mm3(eb, jnp.concatenate([w, zero], axis=0), 1, 0)
    lowrow = jnp.where(hcol < HB, eb, -e21)
    inverse = pltpu.roll(jnp.concatenate([ea, lowrow], axis=0), HB, 1)
    upper = jnp.concatenate([jnp.where(hcol < HB, jnp.where(hrow <= hcol, xa, 0.0), ua),
                             jnp.where(hcol - HB >= hrow, xb, 0.0)], axis=0)
    return upper.T, inverse

def layout(nblock):
    nsuper = nblock // 2
    sizes = [BS * (2 * nblock - 4 * j - 1) for j in range(nsuper)]
    begins, chunks, pads, at = {}, [], [], 0
    for group, pieces in zip(((0, nsuper - 1), (1, 2), range(3, nsuper - 1)), PIECES):
        base = at
        for j in group:
            begins[j] = at
            at += sizes[j]
        if base == 0:
            rhs = at
            at += nblock
        pads.append((at, base + UNIT * sum(pieces)))
        at = base
        for piece in pieces:
            chunks.append((at, UNIT * piece))
            at += UNIT * piece
    return begins, rhs, chunks, pads, at


def sides(nblock, begins, j):
    left = begins[j] - j * SB
    return left, left + BS * (nblock - 2 * j - 1)


def factor_all(nblock, begins, rhs, packed, factor_ref, z_ref, wh, wl, tiles, y, inv_h, inv_l, hook):
    nsuper = nblock // 2
    spare = nsuper * (nsuper + 1) // 2

    def at(ii):
        return pl.ds(pl.multiple_of(ii * SB, SB), SB)

    def spot(j, ii):
        return (j * (2 * nsuper + 1 - j)) // 2 + ii - j

    def both(j, ii):
        k = spot(j, ii)
        return wh[k], wl[k]

    def fetch(kk):
        if isinstance(kk, int):
            first, second = sides(nblock, begins, kk)
        else:
            first, second = (jnp.int32(v) for v in sides(nblock, begins, 1))
            for j in range(2, nsuper):
                left, right = sides(nblock, begins, j)
                first = jnp.where(kk == j, left, first)
                second = jnp.where(kk == j, right, second)

        @pl.loop(kk, nsuper)
        def _(ii):
            for side, begin in enumerate((first, second)):
                rows = pl.ds(pl.multiple_of(begin + ii * SB, BS), SB)
                tiles[kk % 3, at(ii), side * BS : (side + 1) * BS] = packed[rows, :]

    def fetch_first(low, high):
        @pl.loop(low, high)
        def _(ii):
            for side in range(2):
                rows = pl.ds(pl.multiple_of(2 * SB * ii - BS + side * SB, BS), SB)
                tiles[0, at(ii), side * BS : (side + 1) * BS] = packed[rows, :]

    row = lax.broadcasted_iota(jnp.int32, (BS, BS), 0)
    col = lax.broadcasted_iota(jnp.int32, (BS, BS), 1)
    zero = jnp.zeros((BS, BS), jnp.float32)
    for side in range(3):
        tiles[side, nsuper * SB :, :] = jnp.zeros((SB, SB), jnp.float32)
    y[nsuper] = jnp.zeros((SUB, SB), jnp.float32)
    tiles[0, 0:SB, 0:BS] = packed[0:SB, :]
    tiles[0, 0:SB, BS:SB] = packed[BS : BS + SB, :]
    fetch_first(1, 2)

    def pivot(kk, here, fill):
        diag = tiles[here, at(kk), :]
        la, ea = chol_block(diag[0:BS, 0:BS], fill)
        eas = split(ea)
        l21 = mm3(diag[BS:SB, 0:BS], eas, 1, 1)
        l21s = split(l21)
        lb, eb = chol_block(diag[BS:SB, BS:SB] - mm3(l21s, l21s, 1, 1), fill)
        ec = -mm3(eb, mm3(l21s, eas, 1, 0), 1, 0)
        inv = split(jnp.concatenate(
            [jnp.concatenate([ea, zero], axis=1), jnp.concatenate([ec, eb], axis=1)], axis=0))
        low = jnp.concatenate(
            [jnp.concatenate([la, zero], axis=1), jnp.concatenate([l21, lb], axis=1)], axis=0)
        k = spot(kk, kk)
        wh[k], wl[k] = split(low)
        inv_h[kk], inv_l[kk] = inv
        return inv

    early = iter(range(2 * SUB))
    inv = pivot(0, 0, lambda: hook("pivot%d" % next(early)))
    side = split(mm3(tiles[0, at(1), :], inv, 1, 1))
    wh[1], wl[1] = side
    hook("solved")
    fetch_first(2, nsuper)
    for b in range(nblock):
        y[b // 2, 0:1, (b % 2) * BS : (b % 2 + 1) * BS] = packed[rhs + b : rhs + b + 1, :]
        if b % 2 == 0:
            y[b // 2, 1:SUB, :] = jnp.zeros((SUB - 1, SB), jnp.float32)
    y[0] = mm3(y[0], (inv_h[0], inv_l[0]), 1, 1)
    fetch(1)
    side = both(0, 1)
    tiles[1, at(1), :] = tiles[1, at(1), :] - mm3(side, side, 1, 1)
    fetch(2)

    @pl.loop(1, nsuper)
    def _(kk):
        last = kk - 1
        prev, here, there = (kk + 2) % 3, kk % 3, (kk + 1) % 3
        rest = nsuper - 1 - kk
        final = nsuper - 1
        cursor = [kk + 1, 0]

        def follow(n):
            ii = kk + 1 + n
            valid = ii < nsuper
            value = split(
                mm3(tiles[prev, at(jnp.minimum(ii, final)), :], (inv_h[last], inv_l[last]), 1, 1)
            )
            k = jnp.where(valid, spot(last, ii), spare)
            wh[k], wl[k] = value
            k = jnp.where(valid, ii, nsuper)
            y[k] = y[k] - mm3(y[last], value, 1, 1)

        def update(n):
            first = n < rest
            ii2, j2 = cursor
            valid = first | (ii2 < nsuper)
            j = jnp.where(valid, jnp.where(first, last, j2), 0)
            ii = jnp.where(valid, jnp.where(first, kk + 1 + n, ii2), 0)
            other = jnp.where(valid, jnp.where(first, kk, kk + 1), 0)
            side = jnp.where(valid, jnp.where(first, here, there), 0)
            dest = jnp.where(valid, ii, nsuper)
            moved = jnp.where(first, j2, j2 + 1)
            done = jnp.logical_not(first) & (moved >= kk)
            cursor[0] = jnp.where(done, ii2 + 1, ii2)
            cursor[1] = jnp.where(done, 0, moved)
            tiles[side, at(dest), :] = tiles[side, at(dest), :] - mm3(both(j, ii), both(j, other), 1, 1)

        plan = [[functools.partial(follow, 2 * n), functools.partial(follow, 2 * n + 1)] for n in range(3)]
        plan += [[functools.partial(update, 2 * n), functools.partial(update, 2 * n + 1)] for n in range(3)]
        plan += [[functools.partial(update, n)] for n in range(6, 2 * SUB)]
        steps = iter(plan)

        def fill():
            for f in next(steps):
                f()

        for step in (1, 2):

            @pl.when(kk == step)
            def _():
                hook("first%d" % step)

        ykk = y[kk] - mm3(y[last], both(last, kk), 1, 1)
        inv = pivot(kk, here, fill)
        y[kk] = mm3(ykk, inv, 1, 1)
        value = split(mm3(tiles[here, at(jnp.minimum(kk + 1, final)), :], inv, 1, 1))
        k = jnp.where(kk < final, spot(kk, kk + 1), spare)
        wh[k], wl[k] = value
        dest = jnp.where(kk < final, kk + 1, nsuper)
        tiles[there, at(dest), :] = tiles[there, at(dest), :] - mm3(value, value, 1, 1)

        for step in (1, 2):

            @pl.when(kk == step)
            def _():
                hook("last%d" % step)

        @pl.when(kk + 2 < nsuper)
        def _():
            fetch(kk + 2)

    state = [y[j] for j in range(nsuper)]
    for kk in reversed(range(nsuper)):
        state[kk] = mm3(state[kk], (inv_h[kk], inv_l[kk]), 1, 0)
        x = split(state[kk])
        for j in reversed(range(kk)):
            state[j] = state[j] - mm3(x, both(j, kk), 1, 0)
    for b in range(nblock):
        z_ref[b : b + 1, :] = state[b // 2][0:1, (b % 2) * BS : (b % 2 + 1) * BS]

    per_row, per_col = factor_ref.shape[0], factor_ref.shape[2] // BS
    rows_of, cols_of = nblock // per_row, nblock // per_col
    for r in range(per_row):
        for c in range(per_col):
            rb = r * rows_of + lax.axis_index("gx")
            cb = c * cols_of + lax.axis_index("gy")
            k = spot(cb // 2, jnp.maximum(rb // 2, cb // 2))
            rows = pl.ds(pl.multiple_of((rb % 2) * BS, BS), BS)
            wide = wh[k, rows, :].astype(jnp.float32) + wl[k, rows, :].astype(jnp.float32)
            block = jnp.where(cb % 2 == 0, wide[:, :BS], wide[:, BS:])
            inside = row + rb * BS >= col + cb * BS
            factor_ref[r, :, c * BS : (c + 1) * BS] = jnp.where(inside, block, 0.0)


def make_design(nblock, blocks_ref, coef_ref, design, wide):
    slots, rows = blocks_ref.shape
    chunk = 128

    @pl.loop(0, rows // chunk)
    def _(t):
        at = pl.ds(pl.multiple_of(t * chunk, chunk), chunk)
        idx = blocks_ref[:, at]
        idx = jnp.concatenate([idx] * (SUB // slots), axis=0).T
        labels = [jnp.broadcast_to(idx[:, s : s + 1], (chunk, BS)) for s in range(slots)]
        span = chunk * slots
        wide[...] = coef_ref[pl.ds(pl.multiple_of(t * span, span), span), :].astype(jnp.float32)
        values = [wide[pl.ds(s, chunk, stride=slots), :] for s in range(slots)]
        for b in range(nblock):
            total = jnp.where(labels[0] == b, values[0], 0.0)
            for s in range(1, slots):
                total = jnp.where(labels[s] == b, values[s], total)
            design[at, b * BS : (b + 1) * BS] = total.astype(jnp.bfloat16)


def make_rhs(nblock, scale, base, res_ref, design, term):
    rows = res_ref.shape[1]
    res = res_ref[...]
    high = res.astype(jnp.bfloat16)
    rest = res - high.astype(jnp.float32)
    mid = rest.astype(jnp.bfloat16)
    low = (rest - mid.astype(jnp.float32)).astype(jnp.bfloat16)
    row = lax.broadcasted_iota(jnp.int32, (16, rows), 0)
    parts = jnp.where(
        row == 0,
        high.astype(jnp.float32),
        jnp.where(
            row == 1,
            mid.astype(jnp.float32),
            jnp.where(row == 2, low.astype(jnp.float32), 0.0),
        ),
    ).astype(jnp.bfloat16)
    for b in range(nblock // 2):
        part = mm(parts, design[:, b * SB : (b + 1) * SB], 1, 0, None)
        total = jnp.sum(part, axis=0, keepdims=True) * scale
        term[base + 2 * b : base + 2 * b + 1, :] = total[:, :BS]
        term[base + 2 * b + 1 : base + 2 * b + 2, :] = total[:, BS:]


def gram_panel(nblock, scale, jj, begins, design, term, low, high):
    first, second = sides(nblock, begins, jj)
    right = design[:, jj * SB : (jj + 1) * SB]
    if low == jj:
        begin = begins[jj]
        block = mm(right, right, 0, 0, None) * scale
        term[begin : begin + SB, :] = block[:, :BS]
        begin = SB if jj == 0 else second + jj * SB + BS
        term[begin : begin + BS, :] = block[BS:, BS:]

    @pl.loop(max(low, jj + 1), high)
    def _(ii):
        left = design[:, pl.ds(pl.multiple_of(ii * SB, SB), SB)]
        block = mm(left, design[:, jj * SB : (jj + 1) * SB], 0, 0, None) * scale
        near = 2 * SB * ii - BS if jj == 0 else first + ii * SB
        far = 2 * SB * ii + BS if jj == 0 else second + ii * SB
        term[pl.ds(pl.multiple_of(near, BS), SB), :] = block[:, :BS]
        term[pl.ds(pl.multiple_of(far, BS), SB), :] = block[:, BS:]


def exchanger(chunks, term_ref, out_ref, acc, recv, sends, recvs):
    gx, gy, gz = lax.axis_index("gx"), lax.axis_index("gy"), lax.axis_index("gz")
    x, ylo = gx % 4, gx // 4
    z, core = gy // 2, gy % 2

    def flip(v):
        return v + 1 - 2 * (v % 2)

    def gray(v):
        return (v % 2) + (v // 2) - 2 * (v % 2) * (v // 2)

    y = 2 * gz + ylo
    ynext = 4 * (1 - ylo)
    partner = [
        {"gx": 4 * ylo + flip(x)},
        {"gx": ynext + x},
        {"gy": 2 * flip(z) + core},
        {"gx": 4 * ylo + 3 - x},
        {"gx": ynext + x, "gz": 1 - gz},
        {"gy": 2 * (3 - z) + core},
    ]
    bit = [gray(x), gray(y), gray(z), x // 2, y // 2, z // 2]
    mate = {"gy": 2 * z + 1 - core}
    rows = lambda at, size: pl.ds(pl.multiple_of(at, SUB), size)

    def remote(src, dst, c, s, p, device):
        return pltpu.make_async_remote_copy(
            src_ref=src,
            dst_ref=dst,
            send_sem=sends.at[c, s, p],
            recv_sem=recvs.at[c, s, p],
            device_id=device,
            device_id_type=pl.DeviceIdType.MESH,
        )

    slots, at = {}, 0
    total = sum(size for _, size in chunks) // 2
    for s in range(1, 2 * HALVE + 1):
        slots[s] = at
        at += total >> min(s, HALVE)

    def chunk(c):
        base, size = chunks[c]
        half, part = size // 2, size // 12
        local = [base // 2 + p * part for p in range(6)]
        whole = [base + core * half + p * part for p in range(6)]
        other = [base + (1 - core) * half + p * part for p in range(6)]
        where = []
        for p in range(6):
            steps = [0]
            for level in range(1, HALVE + 1):
                steps.append(steps[-1] + bit[(p + level - 1) % 6] * (part >> level))
            where.append(steps)

        def landing(s, p):
            span = part >> min(s, HALVE)
            slot = slots[s] + ((base // 2) >> min(s, HALVE)) + p * span
            return slice(slot, slot + span)

        def copy(s, p):
            if s == 0:
                src = term_ref.at[rows(other[p], part), :]
                dst = acc.at[local[p] : local[p] + part, :]
                return remote(src, dst, c, 0, p, mate)
            if s <= HALVE:
                span, g = part >> s, (p + s - 1) % 6
                give = where[p][s - 1] + (1 - bit[g]) * span
                src = acc.at[rows(local[p] + give, span), :]
                return remote(src, recv.at[landing(s, p), :], c, s, p, partner[g])
            if s <= 2 * HALVE:
                span, g = part >> HALVE, (p + s - 1) % 6
                src = acc.at[rows(local[p] + where[p][HALVE], span), :]
                return remote(src, recv.at[landing(s, p), :], c, s, p, partner[g])
            level = 3 * HALVE + 1 - s
            block = out_ref.at[rows(whole[p] + where[p][level], part >> level), :]
            device = partner[(p + level - 1) % 6] if level else mate
            return remote(block, block, c, s, p, device)

        def stage(s):
            for p in range(6):
                if s:
                    copy(s - 1, p).wait_recv()
                if s == 1:
                    at = slice(local[p], local[p] + part)
                    acc[at, :] = term_ref[rows(whole[p], part), :] + acc[at, :]
                elif 1 < s <= 2 * HALVE + 1:
                    level = min(s - 1, HALVE)
                    span = part >> level
                    at = rows(local[p] + where[p][level], span)
                    if s - 1 > HALVE:
                        copy(s - 1, p).wait_send()
                    total = acc[at, :] + recv[landing(s - 1, p), :]
                    if s <= 2 * HALVE:
                        acc[at, :] = total
                    else:
                        out_ref[rows(whole[p] + where[p][level], span), :] = total
                if s <= 3 * HALVE + 1:
                    copy(s, p).start()

        def finish():
            for s in range(3 * HALVE + 2):
                if not HALVE < s <= 2 * HALVE:
                    for p in range(6):
                        copy(s, p).wait_send()

        return stage, finish

    runs = [chunk(c) for c in range(len(chunks))]

    def turn(t):
        for (stage, _), rounds in zip(runs, ROUNDS):
            for s, at in enumerate(rounds):
                if at == t:
                    stage(s)

    def finish():
        for _, close in runs:
            close()

    def greet():
        barrier = pltpu.get_barrier_semaphore()
        for device in partner + [mate]:
            pl.semaphore_signal(
                barrier, inc=1, device_id=device, device_id_type=pl.DeviceIdType.MESH
            )

    def meet():
        pl.semaphore_wait(pltpu.get_barrier_semaphore(), len(partner) + 1)

    return turn, finish, greet, meet


ROUNDS = (
    (0, 1, 2, 3, 4, 5, 6, 7, 8, 9, 10, 11),
    (1, 2, 3, 4, 5, 6, 7, 8, 9, 10, 11, 12),
    (2, 3, 4, 5, 6, 7, 8, 9, 10, 11, 12, 13),
    (4, 5, 6, 7, 8, 9, 10, 11, 12, 13, 14, 15),
)
READY = 11
WORK = {0: (0,), 1: (1, 2), 2: (3,), 3: (4, 5, 6)}
TURNS = {'pivot8': (12,), 'solved': (13,), 'first1': (14,), 'last1': (15,)}


def whole_kernel(
    nblock, scale, blocks_ref, coef_ref, res_ref, factor_ref, z_ref,
    design, wide, term, acc, recv, out, wh, wl, tiles, y, inv_h, inv_l, sends, recvs,
):
    nsuper = nblock // 2
    begins, rhs, chunks, pads, _ = layout(nblock)
    turn, finish, greet, meet = exchanger(chunks, term, out, acc, recv, sends, recvs)
    greet()
    for used, end in pads:
        if used < end:
            term[used:end, :] = jnp.zeros((end - used, BS), jnp.float32)

    def gram(j, low=None, high=nsuper):
        gram_panel(nblock, scale, j, begins, design, term, j if low is None else low, high)

    make_design(nblock, blocks_ref, coef_ref, design, wide)
    gram(0, 0, 4)
    meet()
    for t in range(READY + 1):
        turn(t)
        for j in WORK.get(t, ()):
            if j == 0:
                gram(0, 4)
                gram(nsuper - 1)
                make_rhs(nblock, scale, rhs, res_ref, design, term)
            else:
                gram(j)

    def hook(name):
        for t in TURNS.get(name, ()):
            turn(t)

    factor_all(nblock, begins, rhs, out, factor_ref, z_ref, wh, wl, tiles, y, inv_h, inv_l, hook)
    finish()


def on_device(blocks, coefficients, residuals):
    row_count = lax.axis_size("gx")
    col_count = lax.axis_size("gy")
    devices = row_count * col_count * lax.axis_size("gz")
    rows, slots, width = coefficients.shape
    scale = 1.0 / (rows * devices)
    nblock = G // width
    nsuper = nblock // 2
    _, _, chunks, _, total = layout(nblock)
    half = total // 2
    landing = sum(half >> min(s, HALVE) for s in range(1, 2 * HALVE + 1))
    per_row, per_col = nblock // row_count, nblock // col_count
    vmem = pl.BlockSpec(memory_space=pltpu.VMEM)
    sem = pltpu.SemaphoreType.DMA((len(chunks), 3 * HALVE + 2, 6))
    count = nsuper * (nsuper + 1) // 2
    factor, answer = pl.pallas_call(
        functools.partial(whole_kernel, nblock, scale),
        out_shape=(
            jax.ShapeDtypeStruct((per_row, width, per_col * width), jnp.float32),
            jax.ShapeDtypeStruct((nblock, width), jnp.float32),
        ),
        in_specs=[vmem] * 3,
        out_specs=(vmem, vmem),
        scratch_shapes=[
            pltpu.VMEM((rows, G), jnp.bfloat16),
            pltpu.VMEM((BS * slots, width), jnp.float32),
            pltpu.VMEM((total, width), jnp.float32),
            pltpu.VMEM((half, width), jnp.float32),
            pltpu.VMEM((landing, width), jnp.float32),
            pltpu.VMEM((total, width), jnp.float32),
            pltpu.VMEM((count + 1, SB, SB), jnp.bfloat16),
            pltpu.VMEM((count + 1, SB, SB), jnp.bfloat16),
            pltpu.VMEM((3, G + SB, SB), jnp.float32),
            pltpu.VMEM((nsuper + 1, SUB, SB), jnp.float32),
            pltpu.VMEM((nsuper, SB, SB), jnp.bfloat16),
            pltpu.VMEM((nsuper, SB, SB), jnp.bfloat16),
            sem,
            sem,
        ],
        compiler_params=pltpu.CompilerParams(
            vmem_limit_bytes=VMEM_LIMIT, has_side_effects=True, collective_id=0
        ),
    )(blocks.T, coefficients.reshape(rows * slots, width), residuals.reshape(1, rows))
    return (factor.reshape(1, per_row, width, 1, per_col, width), answer)


def solution(mesh):
    in_specs = (
        P(("gx", "gy", "gz"), None),
        P(("gx", "gy", "gz"), None, None),
        P(("gx", "gy", "gz")),
    )
    out_specs = (P("gx", None, None, "gy", None, None), P())
    return jax.shard_map(
        on_device, mesh=mesh, in_specs=in_specs, out_specs=out_specs, check_vma=False
    )
```
